32 devices in a mesh: lat: 8 (over y, x, core), lev: 4 (over z).
Axes of the slice: x: 2, y: 2, z: 4, core: 2. Of those that a mesh axis runs over, the one named last changes fastest.
Arguments:
- fields: float32 [12, 128, 256, 1024], P(None, 'lev', 'lat'), may hold values from -6 to 6
- legendre: bfloat16 [256, 256, 256], P('lat'), as said below
- owner_counts: int32 [8], replicated, may hold values from 1 to 64, 256 in all
Outputs:
- covariance: float32 [512, 128, 128], P('lat', 'lev')
The draws below stay inside these ranges and needn't reach their ends.
Inputs may be any that keep to these rules, and one draw needn't show every extreme that they name: `owner_counts`: each owner holds 1 to 64 total wavenumbers, the counts sum to 256, and some owner holds exactly 64. legendre[lat, m, n] is zero where n < m.
All inputs are finite; a program needn't handle non-finite values.
Results may differ from the reference program's by a relative error of at most 0.0038.
Values may be sent and summed in bfloat16 or wider, within the bound.
A program may use at most 192 MiB of HBM per device.

```python
import math
import jax
import jax.numpy as jnp
import numpy as np
from jax import lax

NLON = 1024
NLAT = 256
MTRUNC = 256
LEV = 128
MEM = 12
NCAP = 64
OWNERS = 8


def draw_legendre(key, part):
    values = jax.random.normal(key, (NLAT, MTRUNC, MTRUNC), jnp.float32) * NLAT ** (-0.5)
    order = jnp.arange(MTRUNC, dtype=jnp.int32)
    keeper = order[None, :] >= order[:, None]
    return jnp.where(keeper[None, :, :], values, jnp.zeros_like(values)).astype(jnp.bfloat16)


def levels(key, extent, shards, smallest, top_value):
    level = 1.0
    for position, parts in shards:
        draws = jax.random.uniform(jax.random.fold_in(jax.random.fold_in(key, 6), position), (parts,), jnp.float32, smallest / len(shards), top_value / len(shards))
        level = level * jnp.repeat(jnp.exp(draws), extent[position] // parts).reshape((-1,) + (1,) * (len(extent) - 1 - position))
    return level


def split_up(number_of, total, reach, slope):
    portions = [(1 << 20) // math.isqrt(rank ** slope) + 1 for rank in range(2, number_of + 1)]
    rest, given = total - reach - (number_of - 1), [1] * (number_of - 1)
    while rest > 0:
        candidates = [i for i in range(number_of - 1) if given[i] < reach]
        mass, remaining = sum([portions[i] for i in candidates]), rest
        for i in candidates:
            addition = min(reach - given[i], max(1, remaining * portions[i] // mass), rest)
            given[i] = given[i] + addition
            rest = rest - addition
    return np.array([reach] + given)


def ragged_sizes(key, number_of, total, most, skew):
    if number_of == 2:
        one = jax.random.randint(key, (), max(1, total - most), min(most, total - 1) + 1)
        return jnp.stack([one, total - one])
    lengths = jnp.asarray(split_up(number_of, total, most, skew), jnp.int32)
    couples = (number_of - 1) // 2
    giver, taker = lengths[1:1 + 2 * couples:2], lengths[2:2 + 2 * couples:2]
    room = jnp.minimum(giver - 1, most - taker)
    moved = jax.random.randint(jax.random.fold_in(key, 1), (couples,), 0, 1 << 20) % (room + 1)
    lengths = lengths.at[1:1 + 2 * couples:2].set(giver - moved).at[2:2 + 2 * couples:2].set(taker + moved)
    return lengths[jax.random.permutation(jax.random.fold_in(key, 2), number_of)]


def normal_values(key, shape, scale, most, split=(), kind=jnp.bfloat16):
    factor_of = levels(key, shape, split, -0.22, 0.18) if split else 1.0
    entries = jax.random.normal(key, shape, jnp.float32) * scale * factor_of
    return jnp.minimum(jnp.maximum(entries, -most), most).astype(kind)


def setup_inputs(seed: int = 0) -> dict:
    splits = jax.random.split(jax.random.key(seed), 4)
    return {
        "fields": normal_values(splits[0], (MEM, LEV, NLAT, NLON), 1.0, 6.0, ((1, 4), (2, 8)), jnp.float32),
        "legendre": draw_legendre(jax.random.fold_in(splits[3], 71), 0),
        "owner_counts": ragged_sizes(splits[2], OWNERS, MTRUNC, NCAP, 2).astype(jnp.int32),
    }


def reference(fields, legendre, owner_counts):
    transform = jnp.fft.rfft(fields, axis=-1)[..., :MTRUNC] * (NLON ** -0.5)
    stacked = jnp.stack([jnp.real(transform), jnp.imag(transform)], axis=0).astype(jnp.float32)
    spectra = jnp.transpose(stacked, (3, 4, 0, 1, 2)).astype(jnp.bfloat16)
    block_size = 32

    def add_block(running, block_id):
        spec_block = lax.dynamic_slice_in_dim(spectra, block_id * block_size, block_size, 1).astype(jnp.float32)
        transform_table_block = lax.dynamic_slice_in_dim(legendre, block_id * block_size, block_size, 1).astype(jnp.float32)
        wavenumber_rows = jnp.einsum('lmqbe,lmn->nmqbe', spec_block, transform_table_block)
        anomaly = (wavenumber_rows - jnp.mean(wavenumber_rows, axis=3, keepdims=True)).astype(jnp.bfloat16)
        anomaly = lax.optimization_barrier(anomaly).astype(jnp.float32)
        return running + jnp.einsum('nmqbe,nmqbk->nek', anomaly, anomaly), None

    blocks_all = jnp.arange(MTRUNC // block_size, dtype=jnp.int32)
    start_sum = jnp.zeros((MTRUNC, LEV, LEV), jnp.float32)
    full, unused = lax.scan(add_block, start_sum, blocks_all)
    wavenumber = jnp.arange(MTRUNC, dtype=jnp.int32)
    divisor = ((MEM - 1) * (2 * wavenumber + 2)).astype(jnp.float32)
    full = full / divisor[:, None, None]
    starts = (jnp.cumsum(owner_counts) - owner_counts).astype(jnp.int32)
    offset = jnp.arange(NCAP, dtype=jnp.int32)
    active_flag = offset[None, :] < owner_counts[:, None]
    slot_index = jnp.where(active_flag, starts[:, None] + offset[None, :], 0).reshape(-1).astype(jnp.int32)
    selected_entries = jnp.take(full, slot_index, axis=0)
    return jnp.where(active_flag.reshape(-1)[:, None, None], selected_entries, jnp.zeros_like(selected_entries))
```

```python
import functools
import math

import jax
import jax.numpy as jnp
import numpy as np
from jax import lax
from jax.experimental import pallas as pl
from jax.experimental.pallas import tpu as pltpu
from jax.sharding import PartitionSpec as P


def fourier_table(points, modes):
    places = jnp.arange(points, dtype=jnp.int32)
    orders = jnp.arange(modes, dtype=jnp.int32)
    phase = places[:, None] * orders[None, :] % points
    angle = phase.astype(jnp.float32) * (2.0 * math.pi / points)
    factor = points ** (-0.5)
    return jnp.stack([jnp.cos(angle) * factor, -jnp.sin(angle) * factor], axis=2)


def plain_on_device(fields, legendre, owner_counts):
    members, lev_rows, lat_rows, points = fields.shape
    modes = legendre.shape[1]
    lev_count = lax.axis_size("lev")
    owners = owner_counts.shape[0]
    capacity = 2 * modes // owners
    dft_table = fourier_table(points, modes)
    spectra = jnp.einsum("belx,xmc->lmcbe", fields, dft_table, precision=lax.Precision.HIGHEST)
    spectra = spectra.reshape(lat_rows, modes, 2 * members * lev_rows).astype(jnp.bfloat16)
    collected_rows, transform_table_rows = (
        lax.all_to_all(spectra, "lat", split_axis=1, concat_axis=0, tiled=True),
        lax.all_to_all(legendre, "lat", split_axis=1, concat_axis=0, tiled=True),
    )
    wavenumber_rows = jnp.einsum(
        "dez,det->tez", collected_rows, transform_table_rows, preferred_element_type=jnp.float32
    )
    resident_modes = wavenumber_rows.shape[1]
    shaped = wavenumber_rows.reshape(modes, resident_modes, 2, members, lev_rows)
    anomaly = (shaped - jnp.mean(shaped, axis=3, keepdims=True)).astype(jnp.bfloat16)
    anomaly = anomaly.reshape(modes, resident_modes, 2 * members * lev_rows)
    starts = jnp.cumsum(owner_counts) - owner_counts
    offset = jnp.arange(capacity, dtype=jnp.int32)
    active_flag = offset[None, :] < owner_counts[:, None]
    slot_index = jnp.where(active_flag, starts[:, None] + offset[None, :], 0).reshape(-1)
    slotted = jnp.take(anomaly, slot_index, axis=0)
    slotted = jnp.where(active_flag.reshape(-1)[:, None, None], slotted, jnp.zeros_like(slotted))
    slotted = slotted[None]
    received = lax.all_to_all(
        lax.all_to_all(slotted, "lat", split_axis=1, concat_axis=2, tiled=True),
        "lev",
        split_axis=2,
        concat_axis=0,
        tiled=True,
    )
    mode_share = received.shape[2]
    blocks = received.reshape(lev_count, capacity, mode_share, 2 * members, lev_rows)
    partial_value = jnp.einsum(
        "esaql,fsaqk->selfk", blocks, blocks, preferred_element_type=jnp.float32
    )
    partial_value = partial_value.reshape(capacity, lev_count * lev_rows, lev_count * lev_rows)
    summed = lax.psum_scatter(partial_value, "lev", scatter_dimension=1, tiled=True)
    owner = lax.axis_index("lat")
    wavenumber = starts[owner] + offset
    live_count = owner_counts[owner]
    divisor = ((members - 1) * (2 * wavenumber + 2)).astype(jnp.float32)
    scaled = summed / divisor[:, None, None]
    return jnp.where((offset < live_count)[:, None, None], scaled, jnp.zeros_like(scaled))


LANES = 128
VMEM_LIMIT = 60 * 1024 * 1024
PAIRS = 2


def split_bf16(values):
    high = values.astype(jnp.bfloat16)
    return high, (values - high.astype(jnp.float32)).astype(jnp.bfloat16)


def folded_tables(points, orders):
    tables = []
    for residues, length in (((1, 3), points // 2), ((0,), points // 4), ((2,), points // 4)):
        m = orders[np.isin(orders % 4, residues)]
        angle = 2.0 * np.pi * ((m[:, None] * np.arange(length)[None, :]) % points) / points
        table = np.concatenate([np.cos(angle), -np.sin(angle)]) * points ** -0.5
        table = table.astype(np.float32)
        high = table.astype(jnp.bfloat16)
        low = (table - high.astype(np.float32)).astype(jnp.bfloat16)
        tables.append(np.stack([high, low]))
    return tables


NT = (((1,), (1,)), ((), ()))
TN = (((0,), (0,)), ((), ()))


def dft_kernel(runs, width, pieces, pairs, *refs):
    field_refs = refs[:pieces]
    odd_ref, zero_ref, two_ref = refs[pieces:pieces + 3]
    out_refs, held = refs[pieces + 3:-1], refs[-1]
    rows, lats, _ = field_refs[0].shape
    quarter = pieces * LANES // 4
    lines = [ref.reshape(rows * lats, LANES) for ref in field_refs]

    def fetch(lat):
        return [
            jnp.concatenate([line[pl.ds(lat + s, rows, lats), :] for s in range(2)], axis=0)
            for line in lines
        ]

    def transform(table_ref, values):
        high, low = split_bf16(values)
        dot = functools.partial(lax.dot_general, dimension_numbers=NT, preferred_element_type=jnp.float32)
        return dot(table_ref[0], high) + (dot(table_ref[1], high) + dot(table_ref[0], low))

    def put(lat, lane, kind, sums):
        done = 0
        for start in runs[kind]:
            held[pl.ds(start * lats + lat, width, lats), :] = (
                sums[done:done + width, lane:lane + LANES]
            )
            done += width

    def step(pair, carry):
        lat = 2 * pair
        values = fetch(lat)
        middle = len(values) // 2
        even = jnp.concatenate([u + v for u, v in zip(values[:middle], values[middle:])], axis=1)
        odd = jnp.concatenate([u - v for u, v in zip(values[:middle], values[middle:])], axis=1)
        parts = (
            transform(odd_ref, odd),
            transform(zero_ref, even[:, :quarter] + even[:, quarter:]),
            transform(two_ref, even[:, :quarter] - even[:, quarter:]),
        )
        for s in range(2):
            for kind, sums in enumerate(parts):
                put(lat + s, s * LANES, kind, sums)
        return carry

    lax.fori_loop(0, lats // 2, step, 0)
    piece = width // pairs

    def emit(index, carry):
        for c, out_ref in enumerate(out_refs):
            base = pl.multiple_of(index * width + c * piece, piece)
            block = held[pl.ds(pl.multiple_of(base * lats, piece * lats), piece * lats), :]
            block = block.astype(jnp.bfloat16).reshape(piece, lats, LANES)
            out_ref[pl.ds(pl.multiple_of(index * piece, piece), piece), :, :] = block
        return carry

    lax.fori_loop(0, out_refs[0].shape[0] // piece, emit, 0)


def dft(fields, lat_count, orders, modes, q, pairs):
    members, lev_rows, lat_rows, points = fields.shape
    rows = members * lev_rows
    lats = 16
    width = modes // lat_count
    kinds = [[i for i in range(lat_count) if i % 4 in r] for r in ((1, 3), (0,), (2,))]
    runs = [[i * width for i in kind] for kind in kinds]
    tables = []
    for t in folded_tables(points, orders):
        count = t.shape[1] // 2
        tables.append(jnp.asarray(t[:, q * count:(q + 1) * count]))
    groups = rows // LANES
    pieces = points // LANES
    return pl.pallas_call(
        functools.partial(dft_kernel, runs, width, pieces, pairs),
        grid=(lat_rows // lats, groups),
        out_shape=[jax.ShapeDtypeStruct((modes // pairs, lat_rows, rows), jnp.bfloat16)] * pairs,
        in_specs=[
            pl.BlockSpec((LANES, lats, LANES), functools.partial(lambda c, l, g: (g, l, c), c))
            for c in range(pieces)
        ]
        + [pl.BlockSpec(t.shape, lambda l, g: (0, 0, 0)) for t in tables],
        out_specs=[pl.BlockSpec((modes // pairs, lats, LANES), lambda l, g: (0, l, g))] * pairs,
        scratch_shapes=[pltpu.VMEM((modes * lats, LANES), jnp.float32)],
        compiler_params=pltpu.CompilerParams(vmem_limit_bytes=VMEM_LIMIT),
        cost_estimate=pl.CostEstimate(flops=15_000_000_000, bytes_accessed=65_000_000, transcendentals=0),
    )(*[fields.reshape(rows, lat_rows, points)] * pieces, *tables)


def legendre_kernel(members, lev_rows, band, x_ref, l_ref, out_ref):
    sources, inner, _, lat_rows, lanes = x_ref.shape
    targets = out_ref.shape[0]
    slots = x_ref.shape[2]
    total = l_ref.shape[-1]
    part = band // targets
    groups = lanes // LANES
    for a in range(slots):
        waves = []
        for i in range(inner):
            x = x_ref[:, i, a].reshape(sources * lat_rows, lanes)
            table = l_ref[:, i, a, :, band * a:]
            table = table.reshape(sources * lat_rows, total - band * a)
            waves.append(lax.dot_general(table, x, TN, preferred_element_type=jnp.float32))
        for t in range(a, slots):
            row = inner * part * (t * (t + 1) // 2 + a)
            for z in range(targets):
                at = (t - a) * band + z * part
                block = jnp.concatenate([w[at:at + part] for w in waves], axis=0)
                parts = [block[:, g * LANES:(g + 1) * LANES] for g in range(groups)]
                total_sum = functools.reduce(jnp.add, parts)
                shift = LANES // 2
                while shift >= lev_rows:
                    total_sum = total_sum + pltpu.roll(total_sum, shift, 1)
                    shift //= 2
                mean = total_sum * (1.0 / members)
                for g in range(groups):
                    out_ref[z, row:row + inner * part, g * LANES:(g + 1) * LANES] = (
                        parts[g] - mean
                    ).astype(jnp.bfloat16)


def covariance_kernel(part, inner, slots, lev_rows, *refs):
    x_refs, out_ref, held = refs[:-2], refs[-2], refs[-1]
    sources, _, lanes = x_refs[0].shape
    pack = LANES // lev_rows
    groups = lanes // LANES
    rows = inner * part
    per_slot = len(x_refs) * groups * pack * rows
    for t in range(slots):
        start = rows * (t * (t + 1) // 2)

        def spread(a, carry):
            row = pl.multiple_of(start + a * rows, rows)
            for c, x_ref in enumerate(x_refs):
                for g in range(groups):
                    parts = [
                        x_ref[v, pl.ds(row, rows), g * LANES:(g + 1) * LANES].astype(jnp.float32)
                        for v in range(sources)
                    ]
                    for s in range(pack):
                        joined = jnp.concatenate(
                            [p[:, s * lev_rows:(s + 1) * lev_rows] for p in parts], axis=1
                        )
                        place = a * per_slot + ((c * groups + g) * pack + s) * rows
                        held[pl.ds(pl.multiple_of(place, rows), rows), :] = joined
            return carry

        lax.fori_loop(0, t + 1, spread, 0)
        depth = (t + 1) * per_slot // part

        def multiply(n, carry):
            for s in range(4):
                each = n * 4 + s
                values = held[pl.ds(each, depth, part), :].astype(jnp.bfloat16)
                product = lax.dot_general(values, values, TN, preferred_element_type=jnp.float32)
                out_ref[each, t] = product.astype(jnp.bfloat16)
            return carry

        lax.fori_loop(0, part // 4, multiply, 0)


def exchange(values, axis):
    return lax.all_to_all(values, axis, split_axis=0, concat_axis=0, tiled=True)


def on_device(lat_count, lev_count, fields, legendre, owner_counts):
    members, lev_rows, lat_rows, points = fields.shape
    modes, totals = legendre.shape[1:]
    owners = owner_counts.shape[0]
    capacity = 2 * modes // owners
    levels = lev_count * lev_rows
    band = lat_count * lev_count
    part = band // lev_count
    slots = modes // band
    rows = members * lev_rows
    pairs = PAIRS
    inner = lev_count // pairs
    orders = np.arange(modes).reshape(slots, lev_count, lat_count).transpose(2, 1, 0).reshape(-1)

    table = legendre.reshape(lat_rows, slots, lev_count, lat_count, totals).transpose(3, 2, 1, 0, 4)
    table = exchange(table, "lat")
    out_rows = inner * part * slots * (slots + 1) // 2
    chunks = []
    for q in range(2):
        for c, spectra in enumerate(dft(fields, lat_count, orders, modes, q, pairs)):
            spectra = exchange(spectra.reshape(lat_count, inner, slots, lat_rows, rows), "lat")
            anomaly = pl.pallas_call(
                functools.partial(legendre_kernel, members, lev_rows, band),
                grid=(1,),
                out_shape=jax.ShapeDtypeStruct((lev_count, out_rows, rows), jnp.bfloat16),
                in_specs=[
                    pl.BlockSpec((lat_count, inner, slots, lat_rows, rows), lambda k: (0, 0, 0, 0, 0)),
                    pl.BlockSpec(
                        (lat_count, inner, slots, lat_rows, totals),
                        functools.partial(lambda c, k: (0, c, 0, 0, 0), c),
                    ),
                ],
                out_specs=pl.BlockSpec((lev_count, out_rows, rows), lambda k: (0, 0, 0)),
                compiler_params=pltpu.CompilerParams(vmem_limit_bytes=VMEM_LIMIT),
                cost_estimate=pl.CostEstimate(
                    flops=2_000_000_000, bytes_accessed=12_000_000, transcendentals=0
                ),
            )(spectra, table)
            chunks.append(exchange(anomaly, "lev"))

    partial_value = pl.pallas_call(
        functools.partial(covariance_kernel, part, inner, slots, lev_rows),
        out_shape=jax.ShapeDtypeStruct((part, slots, levels, levels), jnp.bfloat16),
        in_specs=[pl.BlockSpec(memory_space=pltpu.VMEM)] * len(chunks),
        out_specs=pl.BlockSpec(memory_space=pltpu.VMEM),
        scratch_shapes=[pltpu.VMEM((slots * 2 * members * band, levels), jnp.float32)],
        compiler_params=pltpu.CompilerParams(vmem_limit_bytes=VMEM_LIMIT),
        cost_estimate=pl.CostEstimate(flops=2_000_000_000, bytes_accessed=16_000_000, transcendentals=0),
    )(*chunks)

    partial_value = exchange(partial_value, "lat")
    summed = jnp.sum(partial_value.astype(jnp.float32), axis=0)
    summed = summed.reshape(slots, lev_count, lev_rows, levels).transpose(1, 0, 2, 3)
    full = exchange(summed.astype(jnp.bfloat16), "lev")
    full = full.transpose(1, 0, 2, 3).reshape(slots * lev_count, lev_rows, levels)

    starts = jnp.cumsum(owner_counts) - owner_counts
    share = capacity // lat_count
    here = lax.axis_index("lat")
    first = starts // lat_count + (starts % lat_count > here).astype(jnp.int32)
    rank = first[:, None] + jnp.arange(share, dtype=jnp.int32)[None, :]
    rank = jnp.minimum(rank, slots * lev_count - 1)
    sent = jnp.take(full, rank.reshape(-1), axis=0).reshape(owners, share, lev_rows, levels)
    sent = exchange(sent, "lat").reshape(lat_count * share, lev_rows, levels)
    offset = jnp.arange(capacity, dtype=jnp.int32)
    wavenumber = starts[here] + offset
    place = wavenumber % lat_count * share + offset // lat_count
    live = offset < owner_counts[here]
    chosen = jnp.take(sent, place, axis=0).astype(jnp.float32)
    divisor = ((members - 1) * (2 * wavenumber + 2)).astype(jnp.float32)
    return jnp.where(live[:, None, None], chosen / divisor[:, None, None], jnp.zeros_like(chosen))


def pick(lat_count, lev_count, fields, legendre, owner_counts):
    members, lev_rows, lat_rows, points = fields.shape
    modes = legendre.shape[1]
    fits = (
        lat_rows % 16 == 0
        and members * lev_rows % LANES == 0
        and lev_rows * lev_count == LANES
        and lat_count % 8 == 0
        and lev_count % PAIRS == 0
        and owner_counts.shape[0] == lat_count
        and 2 * modes // lat_count % lat_count == 0
        and modes % (lat_count * lev_count) == 0
    )
    if fits:
        return on_device(lat_count, lev_count, fields, legendre, owner_counts)
    return plain_on_device(fields, legendre, owner_counts)


def solution(mesh):
    return jax.shard_map(
        functools.partial(pick, mesh.shape["lat"], mesh.shape["lev"]),
        mesh=mesh,
        in_specs=(P(None, "lev", "lat", None), P("lat", None, None), P()),
        out_specs=P("lat", "lev", None),
        check_vma=False,
    )
```

```python
import functools
import math

import jax
import jax.numpy as jnp
import numpy as np
from jax import lax
from jax.experimental import pallas as pl
from jax.experimental.pallas import tpu as pltpu
from jax.sharding import PartitionSpec as P


def fourier_table(points, modes):
    places = jnp.arange(points, dtype=jnp.int32)
    orders = jnp.arange(modes, dtype=jnp.int32)
    phase = places[:, None] * orders[None, :] % points
    angle = phase.astype(jnp.float32) * (2.0 * math.pi / points)
    factor = points ** (-0.5)
    return jnp.stack([jnp.cos(angle) * factor, -jnp.sin(angle) * factor], axis=2)


def plain_on_device(fields, legendre, owner_counts):
    members, lev_rows, lat_rows, points = fields.shape
    modes = legendre.shape[1]
    lev_count = lax.axis_size("lev")
    owners = owner_counts.shape[0]
    capacity = 2 * modes // owners
    dft_table = fourier_table(points, modes)
    spectra = jnp.einsum("belx,xmc->lmcbe", fields, dft_table, precision=lax.Precision.HIGHEST)
    spectra = spectra.reshape(lat_rows, modes, 2 * members * lev_rows).astype(jnp.bfloat16)
    collected_rows, transform_table_rows = (
        lax.all_to_all(spectra, "lat", split_axis=1, concat_axis=0, tiled=True),
        lax.all_to_all(legendre, "lat", split_axis=1, concat_axis=0, tiled=True),
    )
    wavenumber_rows = jnp.einsum(
        "dez,det->tez", collected_rows, transform_table_rows, preferred_element_type=jnp.float32
    )
    resident_modes = wavenumber_rows.shape[1]
    shaped = wavenumber_rows.reshape(modes, resident_modes, 2, members, lev_rows)
    anomaly = (shaped - jnp.mean(shaped, axis=3, keepdims=True)).astype(jnp.bfloat16)
    anomaly = anomaly.reshape(modes, resident_modes, 2 * members * lev_rows)
    starts = jnp.cumsum(owner_counts) - owner_counts
    offset = jnp.arange(capacity, dtype=jnp.int32)
    active_flag = offset[None, :] < owner_counts[:, None]
    slot_index = jnp.where(active_flag, starts[:, None] + offset[None, :], 0).reshape(-1)
    slotted = jnp.take(anomaly, slot_index, axis=0)
    slotted = jnp.where(active_flag.reshape(-1)[:, None, None], slotted, jnp.zeros_like(slotted))
    slotted = slotted[None]
    received = lax.all_to_all(
        lax.all_to_all(slotted, "lat", split_axis=1, concat_axis=2, tiled=True),
        "lev",
        split_axis=2,
        concat_axis=0,
        tiled=True,
    )
    mode_share = received.shape[2]
    blocks = received.reshape(lev_count, capacity, mode_share, 2 * members, lev_rows)
    partial_value = jnp.einsum(
        "esaql,fsaqk->selfk", blocks, blocks, preferred_element_type=jnp.float32
    )
    partial_value = partial_value.reshape(capacity, lev_count * lev_rows, lev_count * lev_rows)
    summed = lax.psum_scatter(partial_value, "lev", scatter_dimension=1, tiled=True)
    owner = lax.axis_index("lat")
    wavenumber = starts[owner] + offset
    live_count = owner_counts[owner]
    divisor = ((members - 1) * (2 * wavenumber + 2)).astype(jnp.float32)
    scaled = summed / divisor[:, None, None]
    return jnp.where((offset < live_count)[:, None, None], scaled, jnp.zeros_like(scaled))


LANES = 128
SUB = 8
VMEM_LIMIT = 67_043_328


def split_bf16(values):
    high = values.astype(jnp.bfloat16)
    return high, (values - high.astype(jnp.float32)).astype(jnp.bfloat16)


def folded_tables(points, orders):
    tables = []
    for residues, length in (((1, 3), points // 2), ((0,), points // 4), ((2,), points // 4)):
        m = orders[np.isin(orders % 4, residues)]
        angle = 2.0 * np.pi * ((m[:, None] * np.arange(length)[None, :]) % points) / points
        table = np.concatenate([np.cos(angle), -np.sin(angle)]) * points ** -0.5
        table = table.astype(np.float32)
        high = table.astype(jnp.bfloat16)
        low = (table - high.astype(np.float32)).astype(jnp.bfloat16)
        tables.append(np.stack([high, low]))
    return tables


NT = (((1,), (1,)), ((), ()))
TN = (((0,), (0,)), ((), ()))


def block_of(i, j, lat_count):
    return i * lat_count + j if i % 2 == 0 else (i + 1) * lat_count - 1 - j


def main_kernel(size, *refs):
    lat_count, lev_count, members, lev_rows, totals, counts = size
    f_ref, g_ref, odd_ref, zero_ref, two_ref, out_ref = refs[:6]
    blocks = counts
    t_refs = refs[6:6 + blocks]
    (wide, held, sent, got, out_waves, in_waves, joined_ref, cov) = refs[6 + blocks:14 + blocks]
    (f_sem, own_sem, t_send, t_recv, s_send, s_recv, z_send, z_recv) = refs[14 + blocks:]
    me = lax.axis_index("lat")
    depth = lax.axis_index("lev")
    groups = members * lev_rows // LANES
    lat_rows = f_ref.shape[1] * SUB
    pieces = f_ref.shape[3] // LANES
    halves = 2
    eras = lat_rows // (SUB * halves)
    steps = eras * groups
    pairs = 2 * groups
    pack = LANES // lev_rows
    band = SUB * lev_count
    bands = totals // band
    first_band = [i * lat_count // lev_count for i in range(blocks)]
    base = []
    for i in range(blocks):
        base.append(sum(bands - first_band[b] for b in range(i)) - first_band[i])
    lows = [totals - t_refs[i].shape[-1] for i in range(blocks)]

    def lat_peer(offset):
        return lax.rem(me + offset, lat_count)

    def lev_peer(offset):
        return lax.rem(depth + offset, lev_count)

    def fetch_copy(e, half, c):
        l, g = e // groups * halves + half, lax.rem(e, groups)
        return pltpu.make_async_copy(
            f_ref.at[pl.ds(pl.multiple_of(g * LANES, LANES), LANES), l, :, c * LANES:(c + 1) * LANES],
            wide.at[pl.ds((half * pieces + c) * LANES, LANES)],
            f_sem.at[half],
        )

    def fetch_start(e, half):
        for c in range(pieces):
            fetch_copy(e, half, c).start()

    def fetch_wait(half):
        span = wide.at[pl.ds(half * pieces * LANES, pieces * LANES)]
        pltpu.make_async_copy(span, span, f_sem.at[half]).wait()

    def table_source(i, target):
        row = pl.multiple_of(block_of(i, target, lat_count) * SUB, SUB)
        return g_ref.at[:, pl.ds(row, SUB), lows[i]:]

    def table_send(i):
        for offset in range(1, lat_count):
            target = lat_peer(offset)
            pltpu.make_async_remote_copy(
                src_ref=table_source(i, target),
                dst_ref=t_refs[i].at[me],
                send_sem=t_send.at[i],
                recv_sem=t_recv.at[i],
                device_id={"lat": target},
                device_id_type=pl.DeviceIdType.MESH,
            ).start()

    def own_table(i):
        return pltpu.make_async_copy(table_source(i, me), t_refs[i].at[me], own_sem.at[i])

    def own_spectra(i):
        return pltpu.make_async_copy(sent.at[me, i], got.at[i, me], own_sem.at[blocks + i])

    def spectra_send(i, e):
        for offset in range(1, lat_count):
            target = lat_peer(offset)
            pltpu.make_async_remote_copy(
                src_ref=sent.at[target, i, e],
                dst_ref=got.at[i, me, e],
                send_sem=s_send,
                recv_sem=s_recv.at[i],
                device_id={"lat": target},
                device_id_type=pl.DeviceIdType.MESH,
            ).start()

    def waves_send(place):
        for offset in range(1, lev_count):
            target = lev_peer(offset)
            pltpu.make_async_remote_copy(
                src_ref=out_waves.at[place, target],
                dst_ref=in_waves.at[place, depth],
                send_sem=z_send.at[place],
                recv_sem=z_recv.at[place],
                device_id={"lev": target},
                device_id_type=pl.DeviceIdType.MESH,
            ).start()

    def settle(ref, sem):
        pltpu.make_async_copy(ref, ref, sem).wait()

    for half in range(halves):
        fetch_start(0, half)
    barrier = pltpu.get_barrier_semaphore()
    for offset in range(1, lat_count):
        pl.semaphore_signal(
            barrier, inc=1, device_id={"lat": lat_peer(offset)}, device_id_type=pl.DeviceIdType.MESH
        )
    for offset in range(1, lev_count):
        pl.semaphore_signal(
            barrier, inc=1, device_id={"lev": lev_peer(offset)}, device_id_type=pl.DeviceIdType.MESH
        )
    pl.semaphore_wait(barrier, lat_count + lev_count - 2)
    table_send(0)
    for i in range(blocks):
        own_table(i).start()

    rows_view = wide.reshape(wide.shape[0] * SUB, LANES)
    span = SUB * halves
    block_total = lat_count * blocks

    def transform(table_ref, values):
        high, low = split_bf16(values)
        dot = functools.partial(lax.dot_general, dimension_numbers=NT, preferred_element_type=jnp.float32)
        return dot(table_ref[0], high) + (dot(table_ref[1], high) + dot(table_ref[0], low))

    def put(lat, lane, orders, sums):
        count = sums.shape[0] // 2
        for q in range(2):
            for n, order in enumerate(orders):
                row = q * count + n * block_total
                held[q, pl.ds(order * span + lat, block_total, SUB * span), :] = (
                    sums[row:row + block_total, lane:lane + LANES]
                )

    quarter = pieces * LANES // 4
    kinds = [[r for r in range(SUB) if r % 4 in k] for k in ((1, 3), (0,), (2,))]

    def spectra_step(e, carry):
        for half in range(halves):
            fetch_wait(half)

            def pair_step(pair, carry):
                lat = 2 * pair
                values = [
                    jnp.concatenate(
                        [
                            rows_view[pl.ds((half * pieces + c) * LANES * SUB + lat + s, LANES, SUB), :]
                            for s in range(2)
                        ],
                        axis=0,
                    )
                    for c in range(pieces)
                ]
                middle = pieces // 2
                even = jnp.concatenate([u + v for u, v in zip(values[:middle], values[middle:])], axis=1)
                odd = jnp.concatenate([u - v for u, v in zip(values[:middle], values[middle:])], axis=1)
                parts = (
                    transform(odd_ref, odd),
                    transform(zero_ref, even[:, :quarter] + even[:, quarter:]),
                    transform(two_ref, even[:, :quarter] - even[:, quarter:]),
                )
                for s in range(2):
                    for kind, sums in zip(kinds, parts):
                        put(half * SUB + lat + s, s * LANES, kind, sums)
                return carry

            lax.fori_loop(0, SUB // 2, pair_step, 0)

            @pl.when(e < steps - 1)
            def _():
                fetch_start(e + 1, half)

        def emit(target, carry):
            for i in range(blocks):
                for q in range(2):
                    row = pl.multiple_of((target * blocks + i) * SUB * span, SUB * span)
                    block = held[q, pl.ds(row, SUB * span), :].astype(jnp.bfloat16)
                    sent[target, i, e, :, :, q * LANES:(q + 1) * LANES] = block.reshape(SUB, span, LANES)
            return carry

        lax.fori_loop(0, lat_count, emit, 0)
        spectra_send(0, e)

        @pl.when(e > 0)
        def _():
            spectra_send(1, e - 1)

        return carry

    lax.fori_loop(0, steps, spectra_step, 0)
    for i in range(blocks):
        own_spectra(i).start()
    spectra_send(1, steps - 1)
    table_send(1)
    for i in range(2, blocks):
        table_send(i)

        def rest(e, carry):
            spectra_send(i, e)
            return carry

        lax.fori_loop(0, steps, rest, 0)

    def zero(n, carry):
        cov[n] = jnp.zeros(cov.shape[1:], jnp.float32)
        return carry

    lax.fori_loop(0, cov.shape[0], zero, 0)

    depth_rows = lat_count * lat_rows
    table_base = pairs * totals * SUB

    def legendre_sum(i):
        width = totals - lows[i]
        own_table(i).wait()
        settle(t_refs[i].at[pl.ds(0, lat_count - 1)], t_recv.at[i])

        def spread(source, carry):
            for w in range(width // LANES):
                for era in range(eras):
                    at = table_base // SUB + w * depth_rows + (era * lat_count + source) * span
                    wide[pl.ds(at, span)] = t_refs[i][
                        source, era * span:(era + 1) * span, :, w * LANES:(w + 1) * LANES
                    ].astype(jnp.float32)
            return carry

        lax.fori_loop(0, lat_count, spread, 0)
        own_spectra(i).wait()
        settle(got.at[i, pl.ds(0, lat_count - 1)], s_recv.at[i])
        skip = first_band[i] * band - lows[i]

        def one(m, carry):
            table = jnp.concatenate(
                [
                    rows_view[pl.ds(table_base + w * depth_rows * SUB + m, depth_rows, SUB), :]
                    for w in range(width // LANES)
                ],
                axis=1,
            ).astype(jnp.bfloat16)
            waves = []
            for g in range(groups):
                x = jnp.concatenate(
                    [got[i, :, era * groups + g, m].reshape(lat_count * span, 2 * LANES) for era in range(eras)],
                    axis=0,
                )
                full = lax.dot_general(table, x, TN, preferred_element_type=jnp.float32)
                waves.append(full[skip:])
            for q in range(2):
                parts = [w[:, q * LANES:(q + 1) * LANES] for w in waves]
                total = functools.reduce(jnp.add, parts)
                shift = LANES // 2
                while shift >= lev_rows:
                    total = total + pltpu.roll(total, shift, 1)
                    shift //= 2
                mean = total * (1.0 / members)
                for g in range(groups):
                    rows_view[pl.ds((2 * g + q) * totals * SUB + m, parts[g].shape[0], SUB), :] = parts[g] - mean
            return carry

        lax.fori_loop(0, SUB, one, 0)
        start = block_of(i, me, lat_count) // lev_count

        def emit(t, carry):
            place = base[i] + t
            for w in range(pairs):
                for z in range(lev_count):
                    row = w * totals * SUB + ((t - first_band[i]) * lev_count + z) * SUB * SUB
                    block = rows_view[pl.ds(pl.multiple_of(row, SUB), SUB * SUB), :].astype(jnp.bfloat16)
                    out_waves[place, z, :, w * LANES:(w + 1) * LANES] = block
            waves_send(place)
            in_waves[place, depth] = out_waves[place, depth]
            return carry

        lax.fori_loop(start, bands, emit, 0)

    def covariance(i):
        start = block_of(i, me, lat_count) // lev_count

        def one(t, carry):
            place = base[i] + t
            settle(in_waves.at[place, pl.ds(0, lev_count - 1)], z_recv.at[place])
            for w in range(pairs):
                parts = [
                    in_waves[place, v, :, w * LANES:(w + 1) * LANES].astype(jnp.float32)
                    for v in range(lev_count)
                ]
                for s in range(pack):
                    joined = jnp.concatenate([p[:, s * lev_rows:(s + 1) * lev_rows] for p in parts], axis=1)
                    joined_ref[:, w * pack + s] = joined.reshape(SUB, SUB, LANES)

            def multiply(r, carry):
                x = joined_ref[r].reshape(pairs * pack * SUB, LANES).astype(jnp.bfloat16)
                cov[r * bands + t] += lax.dot_general(x, x, TN, preferred_element_type=jnp.float32)
                return carry

            lax.fori_loop(0, SUB, multiply, 0)
            return carry

        lax.fori_loop(start, bands, one, 0)

    for i in range(blocks):
        legendre_sum(i)
        if i >= blocks - 2:
            covariance(i - blocks + 2)
    for i in range(2, blocks):
        covariance(i)

    def finish(n, carry):
        out_ref[n] = cov[n].astype(jnp.bfloat16)
        return carry

    lax.fori_loop(0, cov.shape[0], finish, 0)
    settle(sent.at[pl.ds(0, lat_count - 1)], s_send)
    for i in range(blocks):
        settle(t_refs[i].at[pl.ds(0, lat_count - 1)], t_send.at[i])

        def drain(t, carry):
            place = base[i] + t
            settle(out_waves.at[place, pl.ds(0, lev_count - 1)], z_send.at[place])
            return carry

        lax.fori_loop(block_of(i, me, lat_count) // lev_count, bands, drain, 0)


def main(lat_count, lev_count, fields, legendre):
    members, lev_rows, lat_rows, points = fields.shape
    modes, totals = legendre.shape[1:]
    rows = members * lev_rows
    groups = rows // LANES
    blocks = modes // (SUB * lat_count)
    bands = totals // (SUB * lev_count)
    levels = lev_count * lev_rows
    span = 2 * SUB
    steps = lat_rows // span * groups
    starts = [block_of(i, j, lat_count) * SUB for j in range(lat_count) for i in range(blocks)]
    orders = np.concatenate([np.array(starts) + r for r in range(SUB)])
    tables = [jnp.asarray(t) for t in folded_tables(points, orders)]
    places = sum(bands - i * lat_count // lev_count for i in range(blocks))
    widths = [totals - i * lat_count * SUB // LANES * LANES for i in range(blocks)]
    wide = max(2 * points, 2 * groups * totals + totals // LANES * lat_count * lat_rows)
    size = (lat_count, lev_count, members, lev_rows, totals, blocks)
    vmem = pl.BlockSpec(memory_space=pltpu.VMEM)
    hbm = pl.BlockSpec(memory_space=pl.ANY)
    return pl.pallas_call(
        functools.partial(main_kernel, size),
        out_shape=jax.ShapeDtypeStruct((SUB * bands, levels, levels), jnp.bfloat16),
        in_specs=[hbm, hbm, vmem, vmem, vmem],
        out_specs=vmem,
        scratch_shapes=[pltpu.VMEM((lat_count, lat_rows, SUB, w), jnp.bfloat16) for w in widths]
        + [
            pltpu.VMEM((wide, SUB, LANES), jnp.float32),
            pltpu.VMEM((2, modes * span, LANES), jnp.float32),
            pltpu.VMEM((lat_count, blocks, steps, SUB, span, 2 * LANES), jnp.bfloat16),
            pltpu.VMEM((blocks, lat_count, steps, SUB, span, 2 * LANES), jnp.bfloat16),
            pltpu.VMEM((places, lev_count, SUB * SUB, 2 * rows), jnp.bfloat16),
            pltpu.VMEM((places, lev_count, SUB * SUB, 2 * rows), jnp.bfloat16),
            pltpu.VMEM((SUB, 2 * groups * (LANES // lev_rows), SUB, LANES), jnp.float32),
            pltpu.VMEM((SUB * bands, levels, levels), jnp.float32),
            pltpu.SemaphoreType.DMA((2,)),
            pltpu.SemaphoreType.DMA((2 * blocks,)),
            pltpu.SemaphoreType.DMA((blocks,)),
            pltpu.SemaphoreType.DMA((blocks,)),
            pltpu.SemaphoreType.DMA,
            pltpu.SemaphoreType.DMA((blocks,)),
            pltpu.SemaphoreType.DMA((places,)),
            pltpu.SemaphoreType.DMA((places,)),
        ],
        compiler_params=pltpu.CompilerParams(
            vmem_limit_bytes=VMEM_LIMIT, collective_id=0, has_side_effects=True
        ),
        cost_estimate=pl.CostEstimate(flops=40_000_000_000, bytes_accessed=80_000_000, transcendentals=0),
    )(fields.reshape(rows, lat_rows // SUB, SUB, points), legendre, *tables)


def exchange(values, axis):
    return lax.all_to_all(values, axis, split_axis=0, concat_axis=0, tiled=True)


def on_device(lat_count, lev_count, fields, legendre, owner_counts):
    members, lev_rows, lat_rows, points = fields.shape
    modes, totals = legendre.shape[1:]
    owners = owner_counts.shape[0]
    capacity = 2 * modes // owners
    levels = lev_count * lev_rows
    band = lat_count * lev_count
    slots = modes // band
    partial_value = main(lat_count, lev_count, fields, legendre)
    partial_value = partial_value.reshape(SUB, slots, levels, levels)

    partial_value = exchange(partial_value, "lat")
    summed = jnp.sum(partial_value.astype(jnp.float32), axis=0)
    summed = summed.reshape(slots, lev_count, lev_rows, levels).transpose(1, 0, 2, 3)
    full = exchange(summed.astype(jnp.bfloat16), "lev")
    full = full.transpose(1, 0, 2, 3).reshape(slots * lev_count, lev_rows, levels)

    starts = jnp.cumsum(owner_counts) - owner_counts
    share = capacity // lat_count
    here = lax.axis_index("lat")
    first = starts // lat_count + (starts % lat_count > here).astype(jnp.int32)
    rank = first[:, None] + jnp.arange(share, dtype=jnp.int32)[None, :]
    rank = jnp.minimum(rank, slots * lev_count - 1)
    sent = jnp.take(full, rank.reshape(-1), axis=0).reshape(owners, share, lev_rows, levels)
    sent = exchange(sent, "lat").reshape(lat_count * share, lev_rows, levels)
    offset = jnp.arange(capacity, dtype=jnp.int32)
    wavenumber = starts[here] + offset
    place = wavenumber % lat_count * share + offset // lat_count
    live = offset < owner_counts[here]
    chosen = jnp.take(sent, place, axis=0).astype(jnp.float32)
    divisor = ((members - 1) * (2 * wavenumber + 2)).astype(jnp.float32)
    return jnp.where(live[:, None, None], chosen / divisor[:, None, None], jnp.zeros_like(chosen))


def pick(lat_count, lev_count, fields, legendre, owner_counts):
    members, lev_rows, lat_rows, points = fields.shape
    modes = legendre.shape[1]
    fits = (
        lat_rows % 16 == 0
        and members * lev_rows % LANES == 0
        and lev_rows * lev_count == LANES
        and lat_count == SUB
        and modes % (2 * SUB * lat_count) == 0
        and owner_counts.shape[0] == lat_count
        and 2 * modes // lat_count % lat_count == 0
        and modes % (lat_count * lev_count) == 0
    )
    if fits:
        return on_device(lat_count, lev_count, fields, legendre, owner_counts)
    return plain_on_device(fields, legendre, owner_counts)


def solution(mesh):
    return jax.shard_map(
        functools.partial(pick, mesh.shape["lat"], mesh.shape["lev"]),
        mesh=mesh,
        in_specs=(P(None, "lev", "lat", None), P("lat", None, None), P()),
        out_specs=P("lat", "lev", None),
        check_vma=False,
    )
```

```python
import functools
import math

import jax
import jax.numpy as jnp
import numpy as np
from jax import lax
from jax.experimental import pallas as pl
from jax.experimental.pallas import tpu as pltpu
from jax.sharding import PartitionSpec as P


def fourier_table(points, modes):
    places = jnp.arange(points, dtype=jnp.int32)
    orders = jnp.arange(modes, dtype=jnp.int32)
    phase = places[:, None] * orders[None, :] % points
    angle = phase.astype(jnp.float32) * (2.0 * math.pi / points)
    factor = points ** (-0.5)
    return jnp.stack([jnp.cos(angle) * factor, -jnp.sin(angle) * factor], axis=2)


def plain_on_device(fields, legendre, owner_counts):
    members, lev_rows, lat_rows, points = fields.shape
    modes = legendre.shape[1]
    lev_count = lax.axis_size("lev")
    owners = owner_counts.shape[0]
    capacity = 2 * modes // owners
    dft_table = fourier_table(points, modes)
    spectra = jnp.einsum("belx,xmc->lmcbe", fields, dft_table, precision=lax.Precision.HIGHEST)
    spectra = spectra.reshape(lat_rows, modes, 2 * members * lev_rows).astype(jnp.bfloat16)
    collected_rows, transform_table_rows = (
        lax.all_to_all(spectra, "lat", split_axis=1, concat_axis=0, tiled=True),
        lax.all_to_all(legendre, "lat", split_axis=1, concat_axis=0, tiled=True),
    )
    wavenumber_rows = jnp.einsum(
        "dez,det->tez", collected_rows, transform_table_rows, preferred_element_type=jnp.float32
    )
    resident_modes = wavenumber_rows.shape[1]
    shaped = wavenumber_rows.reshape(modes, resident_modes, 2, members, lev_rows)
    anomaly = (shaped - jnp.mean(shaped, axis=3, keepdims=True)).astype(jnp.bfloat16)
    anomaly = anomaly.reshape(modes, resident_modes, 2 * members * lev_rows)
    starts = jnp.cumsum(owner_counts) - owner_counts
    offset = jnp.arange(capacity, dtype=jnp.int32)
    active_flag = offset[None, :] < owner_counts[:, None]
    slot_index = jnp.where(active_flag, starts[:, None] + offset[None, :], 0).reshape(-1)
    slotted = jnp.take(anomaly, slot_index, axis=0)
    slotted = jnp.where(active_flag.reshape(-1)[:, None, None], slotted, jnp.zeros_like(slotted))
    slotted = slotted[None]
    received = lax.all_to_all(
        lax.all_to_all(slotted, "lat", split_axis=1, concat_axis=2, tiled=True),
        "lev",
        split_axis=2,
        concat_axis=0,
        tiled=True,
    )
    mode_share = received.shape[2]
    blocks = received.reshape(lev_count, capacity, mode_share, 2 * members, lev_rows)
    partial_value = jnp.einsum(
        "esaql,fsaqk->selfk", blocks, blocks, preferred_element_type=jnp.float32
    )
    partial_value = partial_value.reshape(capacity, lev_count * lev_rows, lev_count * lev_rows)
    summed = lax.psum_scatter(partial_value, "lev", scatter_dimension=1, tiled=True)
    owner = lax.axis_index("lat")
    wavenumber = starts[owner] + offset
    live_count = owner_counts[owner]
    divisor = ((members - 1) * (2 * wavenumber + 2)).astype(jnp.float32)
    scaled = summed / divisor[:, None, None]
    return jnp.where((offset < live_count)[:, None, None], scaled, jnp.zeros_like(scaled))


LANES = 128
SUB = 8
VMEM_LIMIT = 67_043_328


def split_bf16(values):
    high = values.astype(jnp.bfloat16)
    return high, (values - high.astype(jnp.float32)).astype(jnp.bfloat16)


def folded_tables(points, orders):
    tables = []
    for residues, length in (((1, 3), points // 2), ((0,), points // 4), ((2,), points // 4)):
        m = orders[np.isin(orders % 4, residues)]
        angle = 2.0 * np.pi * ((m[:, None] * np.arange(length)[None, :]) % points) / points
        table = np.concatenate([np.cos(angle), -np.sin(angle)]) * points ** -0.5
        table = table.astype(np.float32)
        high = table.astype(jnp.bfloat16)
        low = (table - high.astype(np.float32)).astype(jnp.bfloat16)
        tables.append(np.stack([high, low]))
    return tables


NT = (((1,), (1,)), ((), ()))
TN = (((0,), (0,)), ((), ()))


def block_of(i, j, lat_count):
    return i * lat_count + j if i % 2 == 0 else (i + 1) * lat_count - 1 - j


def main_kernel(size, *refs):
    lat_count, lev_count, members, lev_rows, totals, counts = size
    c_ref, f_ref, g_ref, odd_ref, zero_ref, two_ref, out_ref = refs[:7]
    blocks = counts
    t_refs = refs[7:7 + blocks]
    (wide, held, sent, got, out_waves, in_waves, joined_ref) = refs[7 + blocks:14 + blocks]
    (part_out, part_in, rows_out, rows_in, slots_out, slots_in) = refs[14 + blocks:20 + blocks]
    (f_sem, own_sem, t_send, t_recv, s_send, s_recv, z_send, z_recv) = refs[20 + blocks:28 + blocks]
    (p_send, p_recv, l_send, l_recv, d_send, d_recv) = refs[28 + blocks:]
    me = lax.axis_index("lat")
    depth = lax.axis_index("lev")
    groups = members * lev_rows // LANES
    lat_rows = f_ref.shape[1] * SUB
    pieces = f_ref.shape[3] // LANES
    halves = 2
    eras = lat_rows // (SUB * halves)
    steps = eras * groups
    pairs = 2 * groups
    pack = LANES // lev_rows
    band = SUB * lev_count
    bands = totals // band
    first_band = [i * lat_count // lev_count for i in range(blocks)]
    base = []
    for i in range(blocks):
        base.append(sum(bands - first_band[b] for b in range(i)) - first_band[i])
    lows = [totals - t_refs[i].shape[-1] for i in range(blocks)]

    def lat_peer(offset):
        return lax.rem(me + offset, lat_count)

    def lev_peer(offset):
        return lax.rem(depth + offset, lev_count)

    def fetch_copy(e, half, c):
        l, g = e // groups * halves + half, lax.rem(e, groups)
        return pltpu.make_async_copy(
            f_ref.at[pl.ds(pl.multiple_of(g * LANES, LANES), LANES), l, :, c * LANES:(c + 1) * LANES],
            wide.at[pl.ds((half * pieces + c) * LANES, LANES)],
            f_sem.at[half],
        )

    def fetch_start(e, half):
        for c in range(pieces):
            fetch_copy(e, half, c).start()

    def fetch_wait(half):
        span = wide.at[pl.ds(half * pieces * LANES, pieces * LANES)]
        pltpu.make_async_copy(span, span, f_sem.at[half]).wait()

    def table_source(i, target):
        row = pl.multiple_of(block_of(i, target, lat_count) * SUB, SUB)
        return g_ref.at[:, pl.ds(row, SUB), lows[i]:]

    def table_send(i):
        for offset in range(1, lat_count):
            target = lat_peer(offset)
            pltpu.make_async_remote_copy(
                src_ref=table_source(i, target),
                dst_ref=t_refs[i].at[me],
                send_sem=t_send.at[i],
                recv_sem=t_recv.at[i],
                device_id={"lat": target},
                device_id_type=pl.DeviceIdType.MESH,
            ).start()

    def own_table(i):
        return pltpu.make_async_copy(table_source(i, me), t_refs[i].at[me], own_sem.at[i])

    def own_spectra(i):
        return pltpu.make_async_copy(sent.at[me, i], got.at[i, me], own_sem.at[blocks + i])

    def spectra_send(i, e):
        for offset in range(1, lat_count):
            target = lat_peer(offset)
            pltpu.make_async_remote_copy(
                src_ref=sent.at[target, i, e],
                dst_ref=got.at[i, me, e],
                send_sem=s_send,
                recv_sem=s_recv.at[i],
                device_id={"lat": target},
                device_id_type=pl.DeviceIdType.MESH,
            ).start()

    def waves_send(place):
        for offset in range(1, lev_count):
            target = lev_peer(offset)
            pltpu.make_async_remote_copy(
                src_ref=out_waves.at[place, target],
                dst_ref=in_waves.at[place, depth],
                send_sem=z_send.at[place],
                recv_sem=z_recv.at[place],
                device_id={"lev": target},
                device_id_type=pl.DeviceIdType.MESH,
            ).start()

    def settle(ref, sem):
        pltpu.make_async_copy(ref, ref, sem).wait()

    for half in range(halves):
        fetch_start(0, half)
    barrier = pltpu.get_barrier_semaphore()
    for offset in range(1, lat_count):
        pl.semaphore_signal(
            barrier, inc=1, device_id={"lat": lat_peer(offset)}, device_id_type=pl.DeviceIdType.MESH
        )
    for offset in range(1, lev_count):
        pl.semaphore_signal(
            barrier, inc=1, device_id={"lev": lev_peer(offset)}, device_id_type=pl.DeviceIdType.MESH
        )
    pl.semaphore_wait(barrier, lat_count + lev_count - 2)
    table_send(0)
    for i in range(blocks):
        own_table(i).start()

    rows_view = wide.reshape(wide.shape[0] * SUB, LANES)
    span = SUB * halves
    block_total = lat_count * blocks

    def transform(table_ref, values):
        high, low = split_bf16(values)
        dot = functools.partial(lax.dot_general, dimension_numbers=NT, preferred_element_type=jnp.float32)
        return dot(table_ref[0], high) + (dot(table_ref[1], high) + dot(table_ref[0], low))

    def put(lat, lane, orders, sums):
        count = sums.shape[0] // 2
        for q in range(2):
            for n, order in enumerate(orders):
                row = q * count + n * block_total
                held[q, pl.ds(order * span + lat, block_total, SUB * span), :] = (
                    sums[row:row + block_total, lane:lane + LANES]
                )

    quarter = pieces * LANES // 4
    kinds = [[r for r in range(SUB) if r % 4 in k] for k in ((1, 3), (0,), (2,))]

    def spectra_step(e, carry):
        for half in range(halves):
            fetch_wait(half)

            def pair_step(pair, carry):
                lat = 2 * pair
                values = [
                    jnp.concatenate(
                        [
                            rows_view[pl.ds((half * pieces + c) * LANES * SUB + lat + s, LANES, SUB), :]
                            for s in range(2)
                        ],
                        axis=0,
                    )
                    for c in range(pieces)
                ]
                middle = pieces // 2
                even = jnp.concatenate([u + v for u, v in zip(values[:middle], values[middle:])], axis=1)
                odd = jnp.concatenate([u - v for u, v in zip(values[:middle], values[middle:])], axis=1)
                parts = (
                    transform(odd_ref, odd),
                    transform(zero_ref, even[:, :quarter] + even[:, quarter:]),
                    transform(two_ref, even[:, :quarter] - even[:, quarter:]),
                )
                for s in range(2):
                    for kind, sums in zip(kinds, parts):
                        put(half * SUB + lat + s, s * LANES, kind, sums)
                return carry

            lax.fori_loop(0, SUB // 2, pair_step, 0)

            @pl.when(e < steps - 1)
            def _():
                fetch_start(e + 1, half)

        def emit(target, carry):
            for i in range(blocks):
                for q in range(2):
                    row = pl.multiple_of((target * blocks + i) * SUB * span, SUB * span)
                    block = held[q, pl.ds(row, SUB * span), :].astype(jnp.bfloat16)
                    sent[target, i, e, :, :, q * LANES:(q + 1) * LANES] = block.reshape(SUB, span, LANES)
            return carry

        lax.fori_loop(0, lat_count, emit, 0)
        spectra_send(0, e)

        @pl.when(e > 0)
        def _():
            spectra_send(1, e - 1)

        return carry

    lax.fori_loop(0, steps, spectra_step, 0)
    for i in range(blocks):
        own_spectra(i).start()
    spectra_send(1, steps - 1)
    table_send(1)
    for i in range(2, blocks):
        table_send(i)

        def rest(e, carry):
            spectra_send(i, e)
            return carry

        lax.fori_loop(0, steps, rest, 0)

    cov = held.reshape(2 * held.shape[1], LANES)

    def cov_rows(r, t):
        return pl.ds(pl.multiple_of((r * bands + t) * LANES, LANES), LANES)

    def zero(n, carry):
        cov[cov_rows(0, n), :] = jnp.zeros((LANES, LANES), jnp.float32)
        return carry

    lax.fori_loop(0, SUB * bands, zero, 0)

    depth_rows = lat_count * lat_rows
    table_base = pairs * totals * SUB

    def legendre_sum(i):
        width = totals - lows[i]
        own_table(i).wait()
        settle(t_refs[i].at[pl.ds(0, lat_count - 1)], t_recv.at[i])

        def spread(source, carry):
            for w in range(width // LANES):
                for era in range(eras):
                    at = table_base // SUB + w * depth_rows + (era * lat_count + source) * span
                    wide[pl.ds(at, span)] = t_refs[i][
                        source, era * span:(era + 1) * span, :, w * LANES:(w + 1) * LANES
                    ].astype(jnp.float32)
            return carry

        lax.fori_loop(0, lat_count, spread, 0)
        own_spectra(i).wait()
        settle(got.at[i, pl.ds(0, lat_count - 1)], s_recv.at[i])
        skip = first_band[i] * band - lows[i]

        def one(m, carry):
            table = jnp.concatenate(
                [
                    rows_view[pl.ds(table_base + w * depth_rows * SUB + m, depth_rows, SUB), :]
                    for w in range(width // LANES)
                ],
                axis=1,
            ).astype(jnp.bfloat16)
            waves = []
            for g in range(groups):
                x = jnp.concatenate(
                    [got[i, :, era * groups + g, m].reshape(lat_count * span, 2 * LANES) for era in range(eras)],
                    axis=0,
                )
                full = lax.dot_general(table, x, TN, preferred_element_type=jnp.float32)
                waves.append(full[skip:])
            for q in range(2):
                parts = [w[:, q * LANES:(q + 1) * LANES] for w in waves]
                total = functools.reduce(jnp.add, parts)
                shift = LANES // 2
                while shift >= lev_rows:
                    total = total + pltpu.roll(total, shift, 1)
                    shift //= 2
                mean = total * (1.0 / members)
                for g in range(groups):
                    rows_view[pl.ds((2 * g + q) * totals * SUB + m, parts[g].shape[0], SUB), :] = parts[g] - mean
            return carry

        lax.fori_loop(0, SUB, one, 0)
        start = block_of(i, me, lat_count) // lev_count

        def emit(t, carry):
            place = base[i] + t
            for w in range(pairs):
                for z in range(lev_count):
                    row = w * totals * SUB + ((t - first_band[i]) * lev_count + z) * SUB * SUB
                    block = rows_view[pl.ds(pl.multiple_of(row, SUB), SUB * SUB), :].astype(jnp.bfloat16)
                    out_waves[place, z, :, w * LANES:(w + 1) * LANES] = block
            waves_send(place)
            in_waves[place, depth] = out_waves[place, depth]
            return carry

        lax.fori_loop(start, bands, emit, 0)

    def covariance(i):
        start = block_of(i, me, lat_count) // lev_count

        def one(t, carry):
            place = base[i] + t
            settle(in_waves.at[place, pl.ds(0, lev_count - 1)], z_recv.at[place])
            for w in range(pairs):
                parts = [
                    in_waves[place, v, :, w * LANES:(w + 1) * LANES].astype(jnp.float32)
                    for v in range(lev_count)
                ]
                for s in range(pack):
                    joined = jnp.concatenate([p[:, s * lev_rows:(s + 1) * lev_rows] for p in parts], axis=1)
                    joined_ref[:, w * pack + s] = joined.reshape(SUB, SUB, LANES)

            def multiply(r, carry):
                x = joined_ref[r].reshape(pairs * pack * SUB, LANES).astype(jnp.bfloat16)
                cov[cov_rows(r, t), :] += lax.dot_general(x, x, TN, preferred_element_type=jnp.float32)
                return carry

            lax.fori_loop(0, SUB, multiply, 0)
            return carry

        lax.fori_loop(start, bands, one, 0)

    def partials(i):
        def one(t, carry):
            for r in range(lat_count):
                part_out[t, r] = cov[cov_rows(r, t), :].astype(jnp.bfloat16)
            for offset in range(1, lat_count):
                target = lat_peer(offset)
                pltpu.make_async_remote_copy(
                    src_ref=part_out.at[t, target],
                    dst_ref=part_in.at[t, me],
                    send_sem=p_send,
                    recv_sem=p_recv.at[t],
                    device_id={"lat": target},
                    device_id_type=pl.DeviceIdType.MESH,
                ).start()
            part_in[t, me] = part_out[t, me]
            return carry

        lax.fori_loop(first_band[i], (first_band + [bands])[i + 1], one, 0)

    def totals_over_lat(low, high):
        def one(t, carry):
            settle(part_in.at[t, pl.ds(0, lat_count - 1)], p_recv.at[t])
            for z in range(lev_count):
                rows = slice(z * lev_rows, (z + 1) * lev_rows)
                total = part_in[t, 0, rows].astype(jnp.float32)
                for source in range(1, lat_count):
                    total = total + part_in[t, source, rows].astype(jnp.float32)
                rows_out[z, t] = total.astype(jnp.bfloat16)
            for offset in range(1, lev_count):
                target = lev_peer(offset)
                pltpu.make_async_remote_copy(
                    src_ref=rows_out.at[target, t],
                    dst_ref=rows_in.at[depth, t],
                    send_sem=l_send,
                    recv_sem=l_recv,
                    device_id={"lev": target},
                    device_id_type=pl.DeviceIdType.MESH,
                ).start()
            rows_in[depth, t] = rows_out[depth, t]
            return carry

        lax.fori_loop(low, high, one, 0)

    for i in range(blocks):
        legendre_sum(i)
        if i >= blocks - 2:
            covariance(i - blocks + 2)
            partials(i - blocks + 2)
    for i in range(2, blocks):
        covariance(i)
        partials(i)
    early = first_band[blocks // 2]
    totals_over_lat(0, early)
    totals_over_lat(early, bands)
    settle(rows_in.at[pl.ds(0, lev_count - 1)], l_recv)

    share = slots_out.shape[1]
    start, mine, count = 0, 0, 0
    for d in range(lat_count):
        held_here = c_ref[d]
        mine = jnp.where(d == me, start, mine)
        count = jnp.where(d == me, held_here, count)
        first = start // lat_count + jnp.where(start % lat_count > me, 1, 0)
        for k in range(share):
            rank = jnp.minimum(first + k, bands * lev_count - 1)
            slots_out[d, k] = rows_in[rank % lev_count, rank // lev_count]
        start = start + held_here
    for offset in range(1, lat_count):
        target = lat_peer(offset)
        pltpu.make_async_remote_copy(
            src_ref=slots_out.at[target],
            dst_ref=slots_in.at[me],
            send_sem=d_send,
            recv_sem=d_recv,
            device_id={"lat": target},
            device_id_type=pl.DeviceIdType.MESH,
        ).start()
    slots_in[me] = slots_out[me]
    settle(slots_in.at[pl.ds(0, lat_count - 1)], d_recv)

    def finish(k, carry):
        for o in range(lat_count):
            offset = k * lat_count + o
            wavenumber = mine + offset
            divisor = ((members - 1) * (2 * wavenumber + 2)).astype(jnp.float32)
            chosen = slots_in[wavenumber % lat_count, k].astype(jnp.float32) / divisor
            out_ref[offset] = jnp.where(offset < count, chosen, jnp.zeros_like(chosen))
        return carry

    lax.fori_loop(0, share, finish, 0)
    settle(part_out.at[:, pl.ds(0, lat_count - 1)], p_send)
    settle(rows_out.at[pl.ds(0, lev_count - 1)], l_send)
    settle(slots_out.at[pl.ds(0, lat_count - 1)], d_send)
    settle(sent.at[pl.ds(0, lat_count - 1)], s_send)
    for i in range(blocks):
        settle(t_refs[i].at[pl.ds(0, lat_count - 1)], t_send.at[i])

        def drain(t, carry):
            place = base[i] + t
            settle(out_waves.at[place, pl.ds(0, lev_count - 1)], z_send.at[place])
            return carry

        lax.fori_loop(block_of(i, me, lat_count) // lev_count, bands, drain, 0)


def on_device(lat_count, lev_count, fields, legendre, owner_counts):
    members, lev_rows, lat_rows, points = fields.shape
    modes, totals = legendre.shape[1:]
    rows = members * lev_rows
    groups = rows // LANES
    blocks = modes // (SUB * lat_count)
    bands = totals // (SUB * lev_count)
    levels = lev_count * lev_rows
    span = 2 * SUB
    steps = lat_rows // span * groups
    starts = [block_of(i, j, lat_count) * SUB for j in range(lat_count) for i in range(blocks)]
    orders = np.concatenate([np.array(starts) + r for r in range(SUB)])
    tables = [jnp.asarray(t) for t in folded_tables(points, orders)]
    places = sum(bands - i * lat_count // lev_count for i in range(blocks))
    widths = [totals - i * lat_count * SUB // LANES * LANES for i in range(blocks)]
    wide = max(2 * points, 2 * groups * totals + totals // LANES * lat_count * lat_rows)
    size = (lat_count, lev_count, members, lev_rows, totals, blocks)
    vmem = pl.BlockSpec(memory_space=pltpu.VMEM)
    hbm = pl.BlockSpec(memory_space=pl.ANY)
    smem = pl.BlockSpec(memory_space=pltpu.SMEM)
    capacity = 2 * modes // owner_counts.shape[0]
    share = capacity // lat_count
    return pl.pallas_call(
        functools.partial(main_kernel, size),
        out_shape=jax.ShapeDtypeStruct((capacity, lev_rows, levels), jnp.float32),
        in_specs=[smem, hbm, hbm, vmem, vmem, vmem],
        out_specs=vmem,
        scratch_shapes=[pltpu.VMEM((lat_count, lat_rows, SUB, w), jnp.bfloat16) for w in widths]
        + [
            pltpu.VMEM((wide, SUB, LANES), jnp.float32),
            pltpu.VMEM((2, modes * span, LANES), jnp.float32),
            pltpu.VMEM((lat_count, blocks, steps, SUB, span, 2 * LANES), jnp.bfloat16),
            pltpu.VMEM((blocks, lat_count, steps, SUB, span, 2 * LANES), jnp.bfloat16),
            pltpu.VMEM((places, lev_count, SUB * SUB, 2 * rows), jnp.bfloat16),
            pltpu.VMEM((places, lev_count, SUB * SUB, 2 * rows), jnp.bfloat16),
            pltpu.VMEM((SUB, 2 * groups * (LANES // lev_rows), SUB, LANES), jnp.float32),
            pltpu.VMEM((bands, lat_count, levels, levels), jnp.bfloat16),
            pltpu.VMEM((bands, lat_count, levels, levels), jnp.bfloat16),
            pltpu.VMEM((lev_count, bands, lev_rows, levels), jnp.bfloat16),
            pltpu.VMEM((lev_count, bands, lev_rows, levels), jnp.bfloat16),
            pltpu.VMEM((lat_count, share, lev_rows, levels), jnp.bfloat16),
            pltpu.VMEM((lat_count, share, lev_rows, levels), jnp.bfloat16),
            pltpu.SemaphoreType.DMA((2,)),
            pltpu.SemaphoreType.DMA((2 * blocks,)),
            pltpu.SemaphoreType.DMA((blocks,)),
            pltpu.SemaphoreType.DMA((blocks,)),
            pltpu.SemaphoreType.DMA,
            pltpu.SemaphoreType.DMA((blocks,)),
            pltpu.SemaphoreType.DMA((places,)),
            pltpu.SemaphoreType.DMA((places,)),
            pltpu.SemaphoreType.DMA,
            pltpu.SemaphoreType.DMA((bands,)),
            pltpu.SemaphoreType.DMA,
            pltpu.SemaphoreType.DMA,
            pltpu.SemaphoreType.DMA,
            pltpu.SemaphoreType.DMA,
        ],
        compiler_params=pltpu.CompilerParams(
            vmem_limit_bytes=VMEM_LIMIT, collective_id=0, has_side_effects=True
        ),
        cost_estimate=pl.CostEstimate(flops=40_000_000_000, bytes_accessed=80_000_000, transcendentals=0),
    )(owner_counts, fields.reshape(rows, lat_rows // SUB, SUB, points), legendre, *tables)


def pick(lat_count, lev_count, fields, legendre, owner_counts):
    members, lev_rows, lat_rows, points = fields.shape
    modes = legendre.shape[1]
    fits = (
        lat_rows % 16 == 0
        and members * lev_rows % LANES == 0
        and lev_rows * lev_count == LANES
        and lat_count == SUB
        and modes % (2 * SUB * lat_count) == 0
        and owner_counts.shape[0] == lat_count
        and 2 * modes // lat_count % lat_count == 0
        and legendre.shape[2] <= 2 * modes
        and modes % (lat_count * lev_count) == 0
    )
    if fits:
        return on_device(lat_count, lev_count, fields, legendre, owner_counts)
    return plain_on_device(fields, legendre, owner_counts)


def solution(mesh):
    return jax.shard_map(
        functools.partial(pick, mesh.shape["lat"], mesh.shape["lev"]),
        mesh=mesh,
        in_specs=(P(None, "lev", "lat", None), P("lat", None, None), P()),
        out_specs=P("lat", "lev", None),
        check_vma=False,
    )
```

```python
import functools
import math

import jax
import jax.numpy as jnp
import numpy as np
from jax import lax
from jax.experimental import pallas as pl
from jax.experimental.pallas import tpu as pltpu
from jax.sharding import PartitionSpec as P


def fourier_table(points, modes):
    places = jnp.arange(points, dtype=jnp.int32)
    orders = jnp.arange(modes, dtype=jnp.int32)
    phase = places[:, None] * orders[None, :] % points
    angle = phase.astype(jnp.float32) * (2.0 * math.pi / points)
    factor = points ** (-0.5)
    return jnp.stack([jnp.cos(angle) * factor, -jnp.sin(angle) * factor], axis=2)


def plain_on_device(fields, legendre, owner_counts):
    members, lev_rows, lat_rows, points = fields.shape
    modes = legendre.shape[1]
    lev_count = lax.axis_size("lev")
    owners = owner_counts.shape[0]
    capacity = 2 * modes // owners
    dft_table = fourier_table(points, modes)
    spectra = jnp.einsum("belx,xmc->lmcbe", fields, dft_table, precision=lax.Precision.HIGHEST)
    spectra = spectra.reshape(lat_rows, modes, 2 * members * lev_rows).astype(jnp.bfloat16)
    collected_rows, transform_table_rows = (
        lax.all_to_all(spectra, "lat", split_axis=1, concat_axis=0, tiled=True),
        lax.all_to_all(legendre, "lat", split_axis=1, concat_axis=0, tiled=True),
    )
    wavenumber_rows = jnp.einsum(
        "dez,det->tez", collected_rows, transform_table_rows, preferred_element_type=jnp.float32
    )
    resident_modes = wavenumber_rows.shape[1]
    shaped = wavenumber_rows.reshape(modes, resident_modes, 2, members, lev_rows)
    anomaly = (shaped - jnp.mean(shaped, axis=3, keepdims=True)).astype(jnp.bfloat16)
    anomaly = anomaly.reshape(modes, resident_modes, 2 * members * lev_rows)
    starts = jnp.cumsum(owner_counts) - owner_counts
    offset = jnp.arange(capacity, dtype=jnp.int32)
    active_flag = offset[None, :] < owner_counts[:, None]
    slot_index = jnp.where(active_flag, starts[:, None] + offset[None, :], 0).reshape(-1)
    slotted = jnp.take(anomaly, slot_index, axis=0)
    slotted = jnp.where(active_flag.reshape(-1)[:, None, None], slotted, jnp.zeros_like(slotted))
    slotted = slotted[None]
    received = lax.all_to_all(
        lax.all_to_all(slotted, "lat", split_axis=1, concat_axis=2, tiled=True),
        "lev",
        split_axis=2,
        concat_axis=0,
        tiled=True,
    )
    mode_share = received.shape[2]
    blocks = received.reshape(lev_count, capacity, mode_share, 2 * members, lev_rows)
    partial_value = jnp.einsum(
        "esaql,fsaqk->selfk", blocks, blocks, preferred_element_type=jnp.float32
    )
    partial_value = partial_value.reshape(capacity, lev_count * lev_rows, lev_count * lev_rows)
    summed = lax.psum_scatter(partial_value, "lev", scatter_dimension=1, tiled=True)
    owner = lax.axis_index("lat")
    wavenumber = starts[owner] + offset
    live_count = owner_counts[owner]
    divisor = ((members - 1) * (2 * wavenumber + 2)).astype(jnp.float32)
    scaled = summed / divisor[:, None, None]
    return jnp.where((offset < live_count)[:, None, None], scaled, jnp.zeros_like(scaled))


LANES = 128
SUB = 8
VMEM_LIMIT = 67_043_328


def split_bf16(values):
    high = values.astype(jnp.bfloat16)
    return high, (values - high.astype(jnp.float32)).astype(jnp.bfloat16)


def folded_tables(points, orders):
    tables = []
    for residues, length in (((1, 3), points // 2), ((0,), points // 4), ((2,), points // 4)):
        m = orders[np.isin(orders % 4, residues)]
        angle = 2.0 * np.pi * ((m[:, None] * np.arange(length)[None, :]) % points) / points
        table = np.concatenate([np.cos(angle), -np.sin(angle)]) * points ** -0.5
        table = table.astype(np.float32)
        high = table.astype(jnp.bfloat16)
        low = (table - high.astype(np.float32)).astype(jnp.bfloat16)
        tables.append(np.stack([high, low]))
    return tables


NT = (((1,), (1,)), ((), ()))
TN = (((0,), (0,)), ((), ()))


def block_of(i, j, lat_count):
    return i * lat_count + j if i % 2 == 0 else (i + 1) * lat_count - 1 - j


def main_kernel(size, *refs):
    lat_count, lev_count, members, lev_rows, totals, counts = size
    c_ref, f_ref, g_ref, odd_ref, zero_ref, two_ref, out_ref = refs[:7]
    blocks = counts
    t_refs = refs[7:7 + blocks]
    (wide, held, sent, got, out_waves, in_waves, joined_ref) = refs[7 + blocks:14 + blocks]
    (part_out, part_in, rows_out, rows_in, slots_out, slots_in) = refs[14 + blocks:20 + blocks]
    (f_sem, own_sem, t_send, t_recv, s_send, s_recv, z_send, z_recv) = refs[20 + blocks:28 + blocks]
    (p_send, p_recv, l_send, l_recv, d_send, d_recv) = refs[28 + blocks:]
    me = lax.axis_index("lat")
    depth = lax.axis_index("lev")
    groups = members * lev_rows // LANES
    lat_rows = f_ref.shape[1] * SUB
    pieces = f_ref.shape[3] // LANES
    halves = 2
    eras = lat_rows // (SUB * halves)
    steps = eras * groups
    pairs = 2 * groups
    pack = LANES // lev_rows
    band = SUB * lev_count
    bands = totals // band
    first_band = [i * lat_count // lev_count for i in range(blocks)]
    base = []
    for i in range(blocks):
        base.append(sum(bands - first_band[b] for b in range(i)) - first_band[i])
    lows = [totals - t_refs[i].shape[-1] for i in range(blocks)]

    def lat_peer(offset):
        return lax.rem(me + offset, lat_count)

    def lev_peer(offset):
        return lax.rem(depth + offset, lev_count)

    def fetch_copy(e, half, c):
        l, g = e // groups * halves + half, lax.rem(e, groups)
        return pltpu.make_async_copy(
            f_ref.at[pl.ds(pl.multiple_of(g * LANES, LANES), LANES), l, :, c * LANES:(c + 1) * LANES],
            wide.at[pl.ds((half * pieces + c) * LANES, LANES)],
            f_sem.at[half],
        )

    def fetch_start(e, half):
        for c in range(pieces):
            fetch_copy(e, half, c).start()

    def fetch_wait(half):
        span = wide.at[pl.ds(half * pieces * LANES, pieces * LANES)]
        pltpu.make_async_copy(span, span, f_sem.at[half]).wait()

    def table_source(i, target):
        row = pl.multiple_of(block_of(i, target, lat_count) * SUB, SUB)
        return g_ref.at[:, pl.ds(row, SUB), lows[i]:]

    def table_send(i):
        for offset in range(1, lat_count):
            target = lat_peer(offset)
            pltpu.make_async_remote_copy(
                src_ref=table_source(i, target),
                dst_ref=t_refs[i].at[me],
                send_sem=t_send.at[i],
                recv_sem=t_recv.at[i],
                device_id={"lat": target},
                device_id_type=pl.DeviceIdType.MESH,
            ).start()

    def own_table(i):
        return pltpu.make_async_copy(table_source(i, me), t_refs[i].at[me], own_sem.at[i])

    def own_spectra(i):
        return pltpu.make_async_copy(sent.at[me, i], got.at[i, me], own_sem.at[blocks + i])

    def spectra_send(i, e):
        for offset in range(1, lat_count):
            target = lat_peer(offset)
            pltpu.make_async_remote_copy(
                src_ref=sent.at[target, i, e],
                dst_ref=got.at[i, me, e],
                send_sem=s_send,
                recv_sem=s_recv.at[i],
                device_id={"lat": target},
                device_id_type=pl.DeviceIdType.MESH,
            ).start()

    def waves_send(place):
        for offset in range(1, lev_count):
            target = lev_peer(offset)
            pltpu.make_async_remote_copy(
                src_ref=out_waves.at[place, target],
                dst_ref=in_waves.at[place, depth],
                send_sem=z_send.at[place],
                recv_sem=z_recv.at[place],
                device_id={"lev": target},
                device_id_type=pl.DeviceIdType.MESH,
            ).start()

    def settle(ref, sem):
        pltpu.make_async_copy(ref, ref, sem).wait()

    for half in range(halves):
        fetch_start(0, half)
    barrier = pltpu.get_barrier_semaphore()
    for offset in range(1, lat_count):
        pl.semaphore_signal(
            barrier, inc=1, device_id={"lat": lat_peer(offset)}, device_id_type=pl.DeviceIdType.MESH
        )
    for offset in range(1, lev_count):
        pl.semaphore_signal(
            barrier, inc=1, device_id={"lev": lev_peer(offset)}, device_id_type=pl.DeviceIdType.MESH
        )
    pl.semaphore_wait(barrier, lat_count + lev_count - 2)
    table_send(0)
    for i in range(blocks):
        own_table(i).start()

    rows_view = wide.reshape(wide.shape[0] * SUB, LANES)
    span = SUB * halves
    block_total = lat_count * blocks

    def transform(table_ref, values):
        high, low = split_bf16(values)
        dot = functools.partial(lax.dot_general, dimension_numbers=NT, preferred_element_type=jnp.float32)
        count = table_ref.shape[1]
        both = dot(table_ref[...].reshape(2 * count, table_ref.shape[2]), high)
        return both[:count] + (both[count:] + dot(table_ref[0], low))

    quarter = pieces * LANES // 4
    kinds = [[r for r in range(SUB) if r % 4 in k] for k in ((1, 3), (0,), (2,))]
    kind_rows = [2 * block_total * sum(len(k) for k in kinds[:n]) for n in range(len(kinds))]

    def spectra_step(e, carry):
        for half in range(halves):
            fetch_wait(half)

            def pair_step(pair, carry):
                lat = 2 * pair
                values = [
                    jnp.concatenate(
                        [
                            rows_view[pl.ds((half * pieces + c) * LANES * SUB + lat + s, LANES, SUB), :]
                            for s in range(2)
                        ],
                        axis=0,
                    )
                    for c in range(pieces)
                ]
                middle = pieces // 2
                even = jnp.concatenate([u + v for u, v in zip(values[:middle], values[middle:])], axis=1)
                odd = jnp.concatenate([u - v for u, v in zip(values[:middle], values[middle:])], axis=1)
                parts = (
                    transform(odd_ref, odd),
                    transform(zero_ref, even[:, :quarter] + even[:, quarter:]),
                    transform(two_ref, even[:, :quarter] - even[:, quarter:]),
                )
                for s in range(2):
                    for row, sums in zip(kind_rows, parts):
                        held[half, pl.ds(row * SUB + lat + s, sums.shape[0], SUB), :] = (
                            sums[:, s * LANES:(s + 1) * LANES]
                        )
                return carry

            lax.fori_loop(0, SUB // 2, pair_step, 0)

            @pl.when(e < steps - 1)
            def _():
                fetch_start(e + 1, half)

        def emit(target, carry):
            for i in range(blocks):
                for first, kind in zip(kind_rows, kinds):
                    for n, order in enumerate(kind):
                        for q in range(2):
                            row = first + (q * len(kind) + n) * block_total + target * blocks + i
                            rows = pl.ds(pl.multiple_of(row * SUB, SUB), SUB)
                            block = jnp.concatenate([held[half, rows, :] for half in range(halves)], axis=0)
                            sent[target, i, e, order, :, q * LANES:(q + 1) * LANES] = block.astype(jnp.bfloat16)
            return carry

        lax.fori_loop(0, lat_count, emit, 0)
        spectra_send(0, e)
        return carry

    lax.fori_loop(0, steps, spectra_step, 0)
    for i in range(blocks):
        own_spectra(i).start()
    for i in range(1, blocks):
        table_send(i)

        def rest(e, carry):
            spectra_send(i, e)
            return carry

        lax.fori_loop(0, steps, rest, 0)

    cov = held.reshape(2 * held.shape[1], LANES)

    def cov_rows(r, t):
        return pl.ds(pl.multiple_of((r * bands + t) * LANES, LANES), LANES)

    def zero(n, carry):
        cov[cov_rows(0, n), :] = jnp.zeros((LANES, LANES), jnp.float32)
        return carry

    lax.fori_loop(0, SUB * bands, zero, 0)

    depth_rows = lat_count * lat_rows
    table_base = pairs * totals * SUB

    def legendre_sum(i):
        width = totals - lows[i]
        own_table(i).wait()
        settle(t_refs[i].at[pl.ds(0, lat_count - 1)], t_recv.at[i])

        def spread(source, carry):
            for w in range(width // LANES):
                for era in range(eras):
                    at = table_base // SUB + w * depth_rows + (era * lat_count + source) * span
                    wide[pl.ds(at, span)] = t_refs[i][
                        source, era * span:(era + 1) * span, :, w * LANES:(w + 1) * LANES
                    ].astype(jnp.float32)
            return carry

        lax.fori_loop(0, lat_count, spread, 0)
        own_spectra(i).wait()
        settle(got.at[i, pl.ds(0, lat_count - 1)], s_recv.at[i])
        skip = first_band[i] * band - lows[i]

        def one(m, carry):
            table = jnp.concatenate(
                [
                    rows_view[pl.ds(table_base + w * depth_rows * SUB + m, depth_rows, SUB), :]
                    for w in range(width // LANES)
                ],
                axis=1,
            ).astype(jnp.bfloat16)
            waves = []
            for g in range(groups):
                x = jnp.concatenate(
                    [got[i, :, era * groups + g, m].reshape(lat_count * span, 2 * LANES) for era in range(eras)],
                    axis=0,
                )
                full = lax.dot_general(table, x, TN, preferred_element_type=jnp.float32)
                waves.append(full[skip:])
            for q in range(2):
                parts = [w[:, q * LANES:(q + 1) * LANES] for w in waves]
                total = functools.reduce(jnp.add, parts)
                shift = LANES // 2
                while shift >= lev_rows:
                    total = total + pltpu.roll(total, shift, 1)
                    shift //= 2
                mean = total * (1.0 / members)
                for g in range(groups):
                    rows_view[pl.ds((2 * g + q) * totals * SUB + m, parts[g].shape[0], SUB), :] = parts[g] - mean
            return carry

        lax.fori_loop(0, SUB, one, 0)
        start = block_of(i, me, lat_count) // lev_count

        def emit(t, carry):
            place = base[i] + t
            for w in range(pairs):
                for z in range(lev_count):
                    row = w * totals * SUB + ((t - first_band[i]) * lev_count + z) * SUB * SUB
                    block = rows_view[pl.ds(pl.multiple_of(row, SUB), SUB * SUB), :].astype(jnp.bfloat16)
                    out_waves[place, z, :, w * LANES:(w + 1) * LANES] = block
            waves_send(place)
            in_waves[place, depth] = out_waves[place, depth]
            return carry

        lax.fori_loop(start, bands, emit, 0)

    def covariance(i):
        start = block_of(i, me, lat_count) // lev_count

        def one(t, carry):
            place = base[i] + t
            settle(in_waves.at[place, pl.ds(0, lev_count - 1)], z_recv.at[place])
            for w in range(pairs):
                parts = [
                    in_waves[place, v, :, w * LANES:(w + 1) * LANES].astype(jnp.float32)
                    for v in range(lev_count)
                ]
                for s in range(pack):
                    joined = jnp.concatenate([p[:, s * lev_rows:(s + 1) * lev_rows] for p in parts], axis=1)
                    joined_ref[:, w * pack + s] = joined.reshape(SUB, SUB, LANES)

            def multiply(r, carry):
                x = joined_ref[r].reshape(pairs * pack * SUB, LANES).astype(jnp.bfloat16)
                cov[cov_rows(r, t), :] += lax.dot_general(x, x, TN, preferred_element_type=jnp.float32)
                return carry

            lax.fori_loop(0, SUB, multiply, 0)
            return carry

        lax.fori_loop(start, bands, one, 0)

    def partials(i):
        def one(t, carry):
            for r in range(lat_count):
                part_out[t, r] = cov[cov_rows(r, t), :].astype(jnp.bfloat16)
            for offset in range(1, lat_count):
                target = lat_peer(offset)
                pltpu.make_async_remote_copy(
                    src_ref=part_out.at[t, target],
                    dst_ref=part_in.at[t, me],
                    send_sem=p_send,
                    recv_sem=p_recv.at[t],
                    device_id={"lat": target},
                    device_id_type=pl.DeviceIdType.MESH,
                ).start()
            part_in[t, me] = part_out[t, me]
            return carry

        lax.fori_loop(first_band[i], (first_band + [bands])[i + 1], one, 0)

    def totals_over_lat(low, high):
        def one(t, carry):
            settle(part_in.at[t, pl.ds(0, lat_count - 1)], p_recv.at[t])
            for z in range(lev_count):
                rows = slice(z * lev_rows, (z + 1) * lev_rows)
                total = part_in[t, 0, rows].astype(jnp.float32)
                for source in range(1, lat_count):
                    total = total + part_in[t, source, rows].astype(jnp.float32)
                rows_out[z, t] = total.astype(jnp.bfloat16)
            for offset in range(1, lev_count):
                target = lev_peer(offset)
                pltpu.make_async_remote_copy(
                    src_ref=rows_out.at[target, t],
                    dst_ref=rows_in.at[depth, t],
                    send_sem=l_send,
                    recv_sem=l_recv,
                    device_id={"lev": target},
                    device_id_type=pl.DeviceIdType.MESH,
                ).start()
            rows_in[depth, t] = rows_out[depth, t]
            return carry

        lax.fori_loop(low, high, one, 0)

    for i in range(blocks):
        legendre_sum(i)
        if i >= blocks - 2:
            covariance(i - blocks + 2)
            partials(i - blocks + 2)
    for i in range(2, blocks):
        covariance(i)
        partials(i)
    early = first_band[blocks // 2]
    totals_over_lat(0, early)
    totals_over_lat(early, bands)
    settle(rows_in.at[pl.ds(0, lev_count - 1)], l_recv)

    share = slots_out.shape[1]
    start, mine, count = 0, 0, 0
    for d in range(lat_count):
        held_here = c_ref[d]
        mine = jnp.where(d == me, start, mine)
        count = jnp.where(d == me, held_here, count)
        first = start // lat_count + jnp.where(start % lat_count > me, 1, 0)
        for k in range(share):
            rank = jnp.minimum(first + k, bands * lev_count - 1)
            slots_out[d, k] = rows_in[rank % lev_count, rank // lev_count]
        start = start + held_here
    for offset in range(1, lat_count):
        target = lat_peer(offset)
        pltpu.make_async_remote_copy(
            src_ref=slots_out.at[target],
            dst_ref=slots_in.at[me],
            send_sem=d_send,
            recv_sem=d_recv,
            device_id={"lat": target},
            device_id_type=pl.DeviceIdType.MESH,
        ).start()
    slots_in[me] = slots_out[me]
    settle(slots_in.at[pl.ds(0, lat_count - 1)], d_recv)

    def finish(k, carry):
        for o in range(lat_count):
            offset = k * lat_count + o
            wavenumber = mine + offset
            divisor = ((members - 1) * (2 * wavenumber + 2)).astype(jnp.float32)
            chosen = slots_in[wavenumber % lat_count, k].astype(jnp.float32) / divisor
            out_ref[offset] = jnp.where(offset < count, chosen, jnp.zeros_like(chosen))
        return carry

    lax.fori_loop(0, share, finish, 0)
    settle(part_out.at[:, pl.ds(0, lat_count - 1)], p_send)
    settle(rows_out.at[pl.ds(0, lev_count - 1)], l_send)
    settle(slots_out.at[pl.ds(0, lat_count - 1)], d_send)
    settle(sent.at[pl.ds(0, lat_count - 1)], s_send)
    for i in range(blocks):
        settle(t_refs[i].at[pl.ds(0, lat_count - 1)], t_send.at[i])

        def drain(t, carry):
            place = base[i] + t
            settle(out_waves.at[place, pl.ds(0, lev_count - 1)], z_send.at[place])
            return carry

        lax.fori_loop(block_of(i, me, lat_count) // lev_count, bands, drain, 0)


def on_device(lat_count, lev_count, fields, legendre, owner_counts):
    members, lev_rows, lat_rows, points = fields.shape
    modes, totals = legendre.shape[1:]
    rows = members * lev_rows
    groups = rows // LANES
    blocks = modes // (SUB * lat_count)
    bands = totals // (SUB * lev_count)
    levels = lev_count * lev_rows
    span = 2 * SUB
    steps = lat_rows // span * groups
    starts = [block_of(i, j, lat_count) * SUB for j in range(lat_count) for i in range(blocks)]
    orders = np.concatenate([np.array(starts) + r for r in range(SUB)])
    tables = [jnp.asarray(t) for t in folded_tables(points, orders)]
    places = sum(bands - i * lat_count // lev_count for i in range(blocks))
    widths = [totals - i * lat_count * SUB // LANES * LANES for i in range(blocks)]
    wide = max(2 * points, 2 * groups * totals + totals // LANES * lat_count * lat_rows)
    size = (lat_count, lev_count, members, lev_rows, totals, blocks)
    vmem = pl.BlockSpec(memory_space=pltpu.VMEM)
    hbm = pl.BlockSpec(memory_space=pl.ANY)
    smem = pl.BlockSpec(memory_space=pltpu.SMEM)
    capacity = 2 * modes // owner_counts.shape[0]
    share = capacity // lat_count
    return pl.pallas_call(
        functools.partial(main_kernel, size),
        out_shape=jax.ShapeDtypeStruct((capacity, lev_rows, levels), jnp.float32),
        in_specs=[smem, hbm, hbm, vmem, vmem, vmem],
        out_specs=vmem,
        scratch_shapes=[pltpu.VMEM((lat_count, lat_rows, SUB, w), jnp.bfloat16) for w in widths]
        + [
            pltpu.VMEM((wide, SUB, LANES), jnp.float32),
            pltpu.VMEM((2, modes * span, LANES), jnp.float32),
            pltpu.VMEM((lat_count, blocks, steps, SUB, span, 2 * LANES), jnp.bfloat16),
            pltpu.VMEM((blocks, lat_count, steps, SUB, span, 2 * LANES), jnp.bfloat16),
            pltpu.VMEM((places, lev_count, SUB * SUB, 2 * rows), jnp.bfloat16),
            pltpu.VMEM((places, lev_count, SUB * SUB, 2 * rows), jnp.bfloat16),
            pltpu.VMEM((SUB, 2 * groups * (LANES // lev_rows), SUB, LANES), jnp.float32),
            pltpu.VMEM((bands, lat_count, levels, levels), jnp.bfloat16),
            pltpu.VMEM((bands, lat_count, levels, levels), jnp.bfloat16),
            pltpu.VMEM((lev_count, bands, lev_rows, levels), jnp.bfloat16),
            pltpu.VMEM((lev_count, bands, lev_rows, levels), jnp.bfloat16),
            pltpu.VMEM((lat_count, share, lev_rows, levels), jnp.bfloat16),
            pltpu.VMEM((lat_count, share, lev_rows, levels), jnp.bfloat16),
            pltpu.SemaphoreType.DMA((2,)),
            pltpu.SemaphoreType.DMA((2 * blocks,)),
            pltpu.SemaphoreType.DMA((blocks,)),
            pltpu.SemaphoreType.DMA((blocks,)),
            pltpu.SemaphoreType.DMA,
            pltpu.SemaphoreType.DMA((blocks,)),
            pltpu.SemaphoreType.DMA((places,)),
            pltpu.SemaphoreType.DMA((places,)),
            pltpu.SemaphoreType.DMA,
            pltpu.SemaphoreType.DMA((bands,)),
            pltpu.SemaphoreType.DMA,
            pltpu.SemaphoreType.DMA,
            pltpu.SemaphoreType.DMA,
            pltpu.SemaphoreType.DMA,
        ],
        compiler_params=pltpu.CompilerParams(
            vmem_limit_bytes=VMEM_LIMIT, collective_id=0, has_side_effects=True
        ),
        cost_estimate=pl.CostEstimate(flops=40_000_000_000, bytes_accessed=80_000_000, transcendentals=0),
    )(owner_counts, fields.reshape(rows, lat_rows // SUB, SUB, points), legendre, *tables)


def pick(lat_count, lev_count, fields, legendre, owner_counts):
    members, lev_rows, lat_rows, points = fields.shape
    modes = legendre.shape[1]
    fits = (
        lat_rows % 16 == 0
        and members * lev_rows % LANES == 0
        and lev_rows * lev_count == LANES
        and lat_count == SUB
        and modes % (2 * SUB * lat_count) == 0
        and owner_counts.shape[0] == lat_count
        and 2 * modes // lat_count % lat_count == 0
        and legendre.shape[2] <= 2 * modes
        and modes % (lat_count * lev_count) == 0
    )
    if fits:
        return on_device(lat_count, lev_count, fields, legendre, owner_counts)
    return plain_on_device(fields, legendre, owner_counts)


def solution(mesh):
    return jax.shard_map(
        functools.partial(pick, mesh.shape["lat"], mesh.shape["lev"]),
        mesh=mesh,
        in_specs=(P(None, "lev", "lat", None), P("lat", None, None), P()),
        out_specs=P("lat", "lev", None),
        check_vma=False,
    )
```

```python
import functools
import math

import jax
import jax.numpy as jnp
import numpy as np
from jax import lax
from jax.experimental import pallas as pl
from jax.experimental.pallas import tpu as pltpu
from jax.sharding import PartitionSpec as P


def fourier_table(points, modes):
    places = jnp.arange(points, dtype=jnp.int32)
    orders = jnp.arange(modes, dtype=jnp.int32)
    phase = places[:, None] * orders[None, :] % points
    angle = phase.astype(jnp.float32) * (2.0 * math.pi / points)
    factor = points ** (-0.5)
    return jnp.stack([jnp.cos(angle) * factor, -jnp.sin(angle) * factor], axis=2)


def plain_on_device(fields, legendre, owner_counts):
    members, lev_rows, lat_rows, points = fields.shape
    modes = legendre.shape[1]
    lev_count = lax.axis_size("lev")
    owners = owner_counts.shape[0]
    capacity = 2 * modes // owners
    dft_table = fourier_table(points, modes)
    spectra = jnp.einsum("belx,xmc->lmcbe", fields, dft_table, precision=lax.Precision.HIGHEST)
    spectra = spectra.reshape(lat_rows, modes, 2 * members * lev_rows).astype(jnp.bfloat16)
    collected_rows, transform_table_rows = (
        lax.all_to_all(spectra, "lat", split_axis=1, concat_axis=0, tiled=True),
        lax.all_to_all(legendre, "lat", split_axis=1, concat_axis=0, tiled=True),
    )
    wavenumber_rows = jnp.einsum(
        "dez,det->tez", collected_rows, transform_table_rows, preferred_element_type=jnp.float32
    )
    resident_modes = wavenumber_rows.shape[1]
    shaped = wavenumber_rows.reshape(modes, resident_modes, 2, members, lev_rows)
    anomaly = (shaped - jnp.mean(shaped, axis=3, keepdims=True)).astype(jnp.bfloat16)
    anomaly = anomaly.reshape(modes, resident_modes, 2 * members * lev_rows)
    starts = jnp.cumsum(owner_counts) - owner_counts
    offset = jnp.arange(capacity, dtype=jnp.int32)
    active_flag = offset[None, :] < owner_counts[:, None]
    slot_index = jnp.where(active_flag, starts[:, None] + offset[None, :], 0).reshape(-1)
    slotted = jnp.take(anomaly, slot_index, axis=0)
    slotted = jnp.where(active_flag.reshape(-1)[:, None, None], slotted, jnp.zeros_like(slotted))
    slotted = slotted[None]
    received = lax.all_to_all(
        lax.all_to_all(slotted, "lat", split_axis=1, concat_axis=2, tiled=True),
        "lev",
        split_axis=2,
        concat_axis=0,
        tiled=True,
    )
    mode_share = received.shape[2]
    blocks = received.reshape(lev_count, capacity, mode_share, 2 * members, lev_rows)
    partial_value = jnp.einsum(
        "esaql,fsaqk->selfk", blocks, blocks, preferred_element_type=jnp.float32
    )
    partial_value = partial_value.reshape(capacity, lev_count * lev_rows, lev_count * lev_rows)
    summed = lax.psum_scatter(partial_value, "lev", scatter_dimension=1, tiled=True)
    owner = lax.axis_index("lat")
    wavenumber = starts[owner] + offset
    live_count = owner_counts[owner]
    divisor = ((members - 1) * (2 * wavenumber + 2)).astype(jnp.float32)
    scaled = summed / divisor[:, None, None]
    return jnp.where((offset < live_count)[:, None, None], scaled, jnp.zeros_like(scaled))


LANES = 128
SUB = 8
VMEM_LIMIT = 67_043_328


def split_bf16(values):
    high = values.astype(jnp.bfloat16)
    return high, (values - high.astype(jnp.float32)).astype(jnp.bfloat16)


def folded_tables(points, orders):
    tables = []
    for residues, length in (((1, 3), points // 2), ((0,), points // 4), ((2,), points // 4)):
        m = orders[np.isin(orders % 4, residues)]
        angle = 2.0 * np.pi * ((m[:, None] * np.arange(length)[None, :]) % points) / points
        table = np.concatenate([np.cos(angle), -np.sin(angle)]) * points ** -0.5
        table = table.astype(np.float32)
        high = table.astype(jnp.bfloat16)
        low = (table - high.astype(np.float32)).astype(jnp.bfloat16)
        tables.append(np.stack([high, low]))
    return tables


NT = (((1,), (1,)), ((), ()))
TN = (((0,), (0,)), ((), ()))


def block_of(i, j, lat_count):
    return i * lat_count + j if i % 2 == 0 else (i + 1) * lat_count - 1 - j


def main_kernel(size, *refs):
    lat_count, lev_count, members, lev_rows, totals, counts = size
    c_ref, f_ref, g_ref, odd_ref, zero_ref, two_ref, out_ref = refs[:7]
    blocks = counts
    t_refs = refs[7:7 + blocks]
    (wide, held, sent, got, out_waves, in_waves, joined_ref) = refs[7 + blocks:14 + blocks]
    (part_out, part_in, rows_out, rows_in, slots_out, slots_in) = refs[14 + blocks:20 + blocks]
    (f_sem, own_sem, t_send, t_recv, s_send, s_recv, z_send, z_recv) = refs[20 + blocks:28 + blocks]
    (p_send, p_recv, l_send, l_recv, d_send, d_recv) = refs[28 + blocks:]
    me = lax.axis_index("lat")
    depth = lax.axis_index("lev")
    groups = members * lev_rows // LANES
    lat_rows = f_ref.shape[1] * SUB
    pieces = f_ref.shape[3] // LANES
    halves = 2
    eras = lat_rows // (SUB * halves)
    steps = eras * groups
    pairs = 2 * groups
    pack = LANES // lev_rows
    band = SUB * lev_count
    bands = totals // band
    first_band = [i * lat_count // lev_count for i in range(blocks)]
    base = []
    for i in range(blocks):
        base.append(sum(bands - first_band[b] for b in range(i)) - first_band[i])
    lows = [totals - t_refs[i].shape[-1] for i in range(blocks)]
    columns = [[(low, totals, i)] for i, low in enumerate(lows)]
    if totals - lows[0] > LANES:
        columns[0] = [(totals - LANES, totals, 0), (lows[0], totals - LANES, blocks)]

    def lat_peer(offset):
        return lax.rem(me + offset, lat_count)

    def lev_peer(offset):
        return lax.rem(depth + offset, lev_count)

    def fetch_copy(e, half, c):
        l, g = e // groups * halves + half, lax.rem(e, groups)
        return pltpu.make_async_copy(
            f_ref.at[pl.ds(pl.multiple_of(g * LANES, LANES), LANES), l, :, c * LANES:(c + 1) * LANES],
            wide.at[pl.ds((half * pieces + c) * LANES, LANES)],
            f_sem.at[half],
        )

    def fetch_start(e, half):
        for c in range(pieces):
            fetch_copy(e, half, c).start()

    def fetch_wait(half):
        span = wide.at[pl.ds(half * pieces * LANES, pieces * LANES)]
        pltpu.make_async_copy(span, span, f_sem.at[half]).wait()

    def table_source(i, target, start, stop):
        row = pl.multiple_of(block_of(i, target, lat_count) * SUB, SUB)
        return g_ref.at[:, pl.ds(row, SUB), start:stop]

    def table_send(i, part):
        start, stop, sem = part
        for offset in range(1, lat_count):
            target = lat_peer(offset)
            pltpu.make_async_remote_copy(
                src_ref=table_source(i, target, start, stop),
                dst_ref=t_refs[i].at[me, :, :, start - lows[i]:stop - lows[i]],
                send_sem=t_send.at[sem],
                recv_sem=t_recv.at[sem],
                device_id={"lat": target},
                device_id_type=pl.DeviceIdType.MESH,
            ).start()

    def own_table(i):
        return pltpu.make_async_copy(table_source(i, me, lows[i], totals), t_refs[i].at[me], own_sem.at[i])

    def own_spectra(i):
        return pltpu.make_async_copy(sent.at[me, i], got.at[i, me], own_sem.at[blocks + i])

    def spectra_send(i, e):
        for offset in range(1, lat_count):
            target = lat_peer(offset)
            pltpu.make_async_remote_copy(
                src_ref=sent.at[target, i, e],
                dst_ref=got.at[i, me, e],
                send_sem=s_send,
                recv_sem=s_recv.at[i],
                device_id={"lat": target},
                device_id_type=pl.DeviceIdType.MESH,
            ).start()

    def waves_copy(place, offset):
        target = lev_peer(offset)
        return pltpu.make_async_remote_copy(
            src_ref=out_waves.at[place, target],
            dst_ref=in_waves.at[place, depth],
            send_sem=z_send.at[place, offset - 1],
            recv_sem=z_recv.at[place],
            device_id={"lev": target},
            device_id_type=pl.DeviceIdType.MESH,
        )

    def for_waves(i, t, act):
        for offset in range(1, lev_count):

            @pl.when(t * lev_count + lev_peer(offset) >= block_of(i, me, lat_count))
            def _():
                act(waves_copy(base[i] + t, offset))

    def settle(ref, sem):
        pltpu.make_async_copy(ref, ref, sem).wait()

    for half in range(halves):
        fetch_start(0, half)
    barrier = pltpu.get_barrier_semaphore()
    for offset in range(1, lat_count):
        pl.semaphore_signal(
            barrier, inc=1, device_id={"lat": lat_peer(offset)}, device_id_type=pl.DeviceIdType.MESH
        )
    for offset in range(1, lev_count):
        pl.semaphore_signal(
            barrier, inc=1, device_id={"lev": lev_peer(offset)}, device_id_type=pl.DeviceIdType.MESH
        )
    pl.semaphore_wait(barrier, lat_count + lev_count - 2)
    table_send(0, columns[0][0])
    for i in range(blocks):
        own_table(i).start()

    rows_view = wide.reshape(wide.shape[0] * SUB, LANES)
    span = SUB * halves
    block_total = lat_count * blocks

    def transform(table_ref, values):
        high, low = split_bf16(values)
        dot = functools.partial(lax.dot_general, dimension_numbers=NT, preferred_element_type=jnp.float32)
        count = table_ref.shape[1]
        both = dot(table_ref[...].reshape(2 * count, table_ref.shape[2]), high)
        return both[:count] + (both[count:] + dot(table_ref[0], low))

    quarter = pieces * LANES // 4
    kinds = [[r for r in range(SUB) if r % 4 in k] for k in ((1, 3), (0,), (2,))]
    kind_rows = [2 * block_total * sum(len(k) for k in kinds[:n]) for n in range(len(kinds))]

    def spectra_step(e, carry):
        for half in range(halves):
            fetch_wait(half)

            def pair_step(pair, carry):
                lat = 2 * pair
                values = [
                    jnp.concatenate(
                        [
                            rows_view[pl.ds((half * pieces + c) * LANES * SUB + lat + s, LANES, SUB), :]
                            for s in range(2)
                        ],
                        axis=0,
                    )
                    for c in range(pieces)
                ]
                middle = pieces // 2
                even = jnp.concatenate([u + v for u, v in zip(values[:middle], values[middle:])], axis=1)
                odd = jnp.concatenate([u - v for u, v in zip(values[:middle], values[middle:])], axis=1)
                parts = (
                    transform(odd_ref, odd),
                    transform(zero_ref, even[:, :quarter] + even[:, quarter:]),
                    transform(two_ref, even[:, :quarter] - even[:, quarter:]),
                )
                for s in range(2):
                    for row, sums in zip(kind_rows, parts):
                        held[half, pl.ds(row * SUB + lat + s, sums.shape[0], SUB), :] = (
                            sums[:, s * LANES:(s + 1) * LANES]
                        )
                return carry

            lax.fori_loop(0, SUB // 2, pair_step, 0)

            @pl.when(e < steps - 1)
            def _():
                fetch_start(e + 1, half)

        def emit(target, carry):
            for i in range(blocks):
                for first, kind in zip(kind_rows, kinds):
                    for n, order in enumerate(kind):
                        for q in range(2):
                            row = first + (q * len(kind) + n) * block_total + target * blocks + i
                            rows = pl.ds(pl.multiple_of(row * SUB, SUB), SUB)
                            block = jnp.concatenate([held[half, rows, :] for half in range(halves)], axis=0)
                            sent[target, i, e, order, :, q * LANES:(q + 1) * LANES] = block.astype(jnp.bfloat16)
            return carry

        lax.fori_loop(0, lat_count, emit, 0)
        spectra_send(0, e)
        return carry

    lax.fori_loop(0, steps, spectra_step, 0)
    for i in range(blocks):
        own_spectra(i).start()
    for part in columns[0][1:]:
        table_send(0, part)
    for i in range(1, blocks):
        for part in columns[i]:
            table_send(i, part)

        def rest(e, carry):
            spectra_send(i, e)
            return carry

        lax.fori_loop(0, steps, rest, 0)

    cov = held.reshape(2 * held.shape[1], LANES)

    def cov_rows(r, t):
        return pl.ds(pl.multiple_of((r * bands + t) * LANES, LANES), LANES)

    def zero(n, carry):
        cov[cov_rows(0, n), :] = jnp.zeros((LANES, LANES), jnp.float32)
        return carry

    lax.fori_loop(0, SUB * bands, zero, 0)

    depth_rows = lat_count * lat_rows
    table_base = pairs * totals * SUB

    def legendre_sum(i):
        own_table(i).wait()
        for n, part in enumerate(columns[i]):
            legendre_part(i, part, n == 0)

    def legendre_part(i, part, first):
        left, right, sem = part
        width = right - left
        low = left - lows[i]
        settle(t_refs[i].at[pl.ds(0, lat_count - 1), :, :, low:low + width], t_recv.at[sem])

        def spread(source, carry):
            for w in range(width // LANES):
                for era in range(eras):
                    at = table_base // SUB + w * depth_rows + (era * lat_count + source) * span
                    wide[pl.ds(at, span)] = t_refs[i][
                        source, era * span:(era + 1) * span, :, low + w * LANES:low + (w + 1) * LANES
                    ].astype(jnp.float32)
            return carry

        lax.fori_loop(0, lat_count, spread, 0)
        if first:
            own_spectra(i).wait()
            settle(got.at[i, pl.ds(0, lat_count - 1)], s_recv.at[i])
        skip = max(first_band[i] * band - left, 0)
        place_row = (left + skip - first_band[i] * band) * SUB

        def one(m, carry):
            table = jnp.concatenate(
                [
                    rows_view[pl.ds(table_base + w * depth_rows * SUB + m, depth_rows, SUB), :]
                    for w in range(width // LANES)
                ],
                axis=1,
            ).astype(jnp.bfloat16)
            waves = []
            for g in range(groups):
                x = jnp.concatenate(
                    [got[i, :, era * groups + g, m].reshape(lat_count * span, 2 * LANES) for era in range(eras)],
                    axis=0,
                )
                full = lax.dot_general(table, x, TN, preferred_element_type=jnp.float32)
                waves.append(full[skip:])
            for q in range(2):
                parts = [w[:, q * LANES:(q + 1) * LANES] for w in waves]
                total = functools.reduce(jnp.add, parts)
                shift = LANES // 2
                while shift >= lev_rows:
                    total = total + pltpu.roll(total, shift, 1)
                    shift //= 2
                mean = total * (1.0 / members)
                for g in range(groups):
                    rows = pl.ds((2 * g + q) * totals * SUB + place_row + m, parts[g].shape[0], SUB)
                    rows_view[rows, :] = parts[g] - mean
            return carry

        lax.fori_loop(0, SUB, one, 0)
        start = jnp.maximum(block_of(i, me, lat_count) // lev_count, left // band)

        def emit(t, carry):
            place = base[i] + t
            for w in range(pairs):
                for z in range(lev_count):
                    row = w * totals * SUB + ((t - first_band[i]) * lev_count + z) * SUB * SUB
                    block = rows_view[pl.ds(pl.multiple_of(row, SUB), SUB * SUB), :].astype(jnp.bfloat16)
                    out_waves[place, z, :, w * LANES:(w + 1) * LANES] = block
            for_waves(i, t, lambda copy: copy.start())
            in_waves[place, depth] = out_waves[place, depth]
            return carry

        lax.fori_loop(start, right // band, emit, 0)

    def covariance(i):
        start = (block_of(i, me, lat_count) + lev_count - 1 - depth) // lev_count

        def one(t, carry):
            place = base[i] + t
            settle(in_waves.at[place, pl.ds(0, lev_count - 1)], z_recv.at[place])
            for w in range(pairs):
                parts = [
                    in_waves[place, v, :, w * LANES:(w + 1) * LANES].astype(jnp.float32)
                    for v in range(lev_count)
                ]
                for s in range(pack):
                    joined = jnp.concatenate([p[:, s * lev_rows:(s + 1) * lev_rows] for p in parts], axis=1)
                    joined_ref[:, w * pack + s] = joined.reshape(SUB, SUB, LANES)

            def multiply(r, carry):
                x = joined_ref[r].reshape(pairs * pack * SUB, LANES).astype(jnp.bfloat16)
                cov[cov_rows(r, t), :] += lax.dot_general(x, x, TN, preferred_element_type=jnp.float32)
                return carry

            lax.fori_loop(0, SUB, multiply, 0)
            return carry

        lax.fori_loop(start, bands, one, 0)

    def partials(i):
        def one(t, carry):
            for r in range(lat_count):
                part_out[t, r] = cov[cov_rows(r, t), :].astype(jnp.bfloat16)
            for offset in range(1, lat_count):
                target = lat_peer(offset)
                pltpu.make_async_remote_copy(
                    src_ref=part_out.at[t, target],
                    dst_ref=part_in.at[t, me],
                    send_sem=p_send,
                    recv_sem=p_recv.at[t],
                    device_id={"lat": target},
                    device_id_type=pl.DeviceIdType.MESH,
                ).start()
            part_in[t, me] = part_out[t, me]
            return carry

        lax.fori_loop(first_band[i], (first_band + [bands])[i + 1], one, 0)

    def totals_over_lat(low, high):
        def one(t, carry):
            settle(part_in.at[t, pl.ds(0, lat_count - 1)], p_recv.at[t])
            for z in range(lev_count):
                rows = slice(z * lev_rows, (z + 1) * lev_rows)
                total = part_in[t, 0, rows].astype(jnp.float32)
                for source in range(1, lat_count):
                    total = total + part_in[t, source, rows].astype(jnp.float32)
                rows_out[z, t] = total.astype(jnp.bfloat16)
            for offset in range(1, lev_count):
                target = lev_peer(offset)
                pltpu.make_async_remote_copy(
                    src_ref=rows_out.at[target, t],
                    dst_ref=rows_in.at[depth, t],
                    send_sem=l_send,
                    recv_sem=l_recv,
                    device_id={"lev": target},
                    device_id_type=pl.DeviceIdType.MESH,
                ).start()
            rows_in[depth, t] = rows_out[depth, t]
            return carry

        lax.fori_loop(low, high, one, 0)

    for i in range(blocks):
        legendre_sum(i)
        if i >= blocks - 2:
            covariance(i - blocks + 2)
            partials(i - blocks + 2)
    for i in range(2, blocks):
        covariance(i)
        partials(i)
    early = first_band[blocks // 2]
    totals_over_lat(0, early)
    totals_over_lat(early, bands)
    settle(rows_in.at[pl.ds(0, lev_count - 1)], l_recv)

    share = slots_out.shape[1]
    start, mine, count = 0, 0, 0
    for d in range(lat_count):
        held_here = c_ref[d]
        mine = jnp.where(d == me, start, mine)
        count = jnp.where(d == me, held_here, count)
        first = start // lat_count + jnp.where(start % lat_count > me, 1, 0)
        for k in range(share):
            rank = jnp.minimum(first + k, bands * lev_count - 1)
            slots_out[d, k] = rows_in[rank % lev_count, rank // lev_count]
        start = start + held_here
    for offset in range(1, lat_count):
        target = lat_peer(offset)
        pltpu.make_async_remote_copy(
            src_ref=slots_out.at[target],
            dst_ref=slots_in.at[me],
            send_sem=d_send,
            recv_sem=d_recv,
            device_id={"lat": target},
            device_id_type=pl.DeviceIdType.MESH,
        ).start()
    slots_in[me] = slots_out[me]
    settle(slots_in.at[pl.ds(0, lat_count - 1)], d_recv)

    def finish(k, carry):
        for o in range(lat_count):
            offset = k * lat_count + o
            wavenumber = mine + offset
            divisor = ((members - 1) * (2 * wavenumber + 2)).astype(jnp.float32)
            chosen = slots_in[wavenumber % lat_count, k].astype(jnp.float32) / divisor
            out_ref[offset] = jnp.where(offset < count, chosen, jnp.zeros_like(chosen))
        return carry

    lax.fori_loop(0, share, finish, 0)
    settle(part_out.at[:, pl.ds(0, lat_count - 1)], p_send)
    settle(rows_out.at[pl.ds(0, lev_count - 1)], l_send)
    settle(slots_out.at[pl.ds(0, lat_count - 1)], d_send)
    settle(sent.at[pl.ds(0, lat_count - 1)], s_send)
    for i in range(blocks):
        for left, right, sem in columns[i]:
            part = t_refs[i].at[pl.ds(0, lat_count - 1), :, :, left - lows[i]:right - lows[i]]
            settle(part, t_send.at[sem])

        def drain(t, carry):
            for_waves(i, t, lambda copy: copy.wait_send())
            return carry

        lax.fori_loop(block_of(i, me, lat_count) // lev_count, bands, drain, 0)


def on_device(lat_count, lev_count, fields, legendre, owner_counts):
    members, lev_rows, lat_rows, points = fields.shape
    modes, totals = legendre.shape[1:]
    rows = members * lev_rows
    groups = rows // LANES
    blocks = modes // (SUB * lat_count)
    bands = totals // (SUB * lev_count)
    levels = lev_count * lev_rows
    span = 2 * SUB
    steps = lat_rows // span * groups
    starts = [block_of(i, j, lat_count) * SUB for j in range(lat_count) for i in range(blocks)]
    orders = np.concatenate([np.array(starts) + r for r in range(SUB)])
    tables = [jnp.asarray(t) for t in folded_tables(points, orders)]
    places = sum(bands - i * lat_count // lev_count for i in range(blocks))
    widths = [totals - i * lat_count * SUB // LANES * LANES for i in range(blocks)]
    wide = max(2 * points, 2 * groups * totals + totals // LANES * lat_count * lat_rows)
    size = (lat_count, lev_count, members, lev_rows, totals, blocks)
    vmem = pl.BlockSpec(memory_space=pltpu.VMEM)
    hbm = pl.BlockSpec(memory_space=pl.ANY)
    smem = pl.BlockSpec(memory_space=pltpu.SMEM)
    capacity = 2 * modes // owner_counts.shape[0]
    share = capacity // lat_count
    return pl.pallas_call(
        functools.partial(main_kernel, size),
        out_shape=jax.ShapeDtypeStruct((capacity, lev_rows, levels), jnp.float32),
        in_specs=[smem, hbm, hbm, vmem, vmem, vmem],
        out_specs=vmem,
        scratch_shapes=[pltpu.VMEM((lat_count, lat_rows, SUB, w), jnp.bfloat16) for w in widths]
        + [
            pltpu.VMEM((wide, SUB, LANES), jnp.float32),
            pltpu.VMEM((2, modes * span, LANES), jnp.float32),
            pltpu.VMEM((lat_count, blocks, steps, SUB, span, 2 * LANES), jnp.bfloat16),
            pltpu.VMEM((blocks, lat_count, steps, SUB, span, 2 * LANES), jnp.bfloat16),
            pltpu.VMEM((places, lev_count, SUB * SUB, 2 * rows), jnp.bfloat16),
            pltpu.VMEM((places, lev_count, SUB * SUB, 2 * rows), jnp.bfloat16),
            pltpu.VMEM((SUB, 2 * groups * (LANES // lev_rows), SUB, LANES), jnp.float32),
            pltpu.VMEM((bands, lat_count, levels, levels), jnp.bfloat16),
            pltpu.VMEM((bands, lat_count, levels, levels), jnp.bfloat16),
            pltpu.VMEM((lev_count, bands, lev_rows, levels), jnp.bfloat16),
            pltpu.VMEM((lev_count, bands, lev_rows, levels), jnp.bfloat16),
            pltpu.VMEM((lat_count, share, lev_rows, levels), jnp.bfloat16),
            pltpu.VMEM((lat_count, share, lev_rows, levels), jnp.bfloat16),
            pltpu.SemaphoreType.DMA((2,)),
            pltpu.SemaphoreType.DMA((2 * blocks,)),
            pltpu.SemaphoreType.DMA((blocks + 1,)),
            pltpu.SemaphoreType.DMA((blocks + 1,)),
            pltpu.SemaphoreType.DMA,
            pltpu.SemaphoreType.DMA((blocks,)),
            pltpu.SemaphoreType.DMA((places, lev_count - 1)),
            pltpu.SemaphoreType.DMA((places,)),
            pltpu.SemaphoreType.DMA,
            pltpu.SemaphoreType.DMA((bands,)),
            pltpu.SemaphoreType.DMA,
            pltpu.SemaphoreType.DMA,
            pltpu.SemaphoreType.DMA,
            pltpu.SemaphoreType.DMA,
        ],
        compiler_params=pltpu.CompilerParams(
            vmem_limit_bytes=VMEM_LIMIT, collective_id=0, has_side_effects=True
        ),
        cost_estimate=pl.CostEstimate(flops=40_000_000_000, bytes_accessed=80_000_000, transcendentals=0),
    )(owner_counts, fields.reshape(rows, lat_rows // SUB, SUB, points), legendre, *tables)


def pick(lat_count, lev_count, fields, legendre, owner_counts):
    members, lev_rows, lat_rows, points = fields.shape
    modes = legendre.shape[1]
    fits = (
        lat_rows % 16 == 0
        and members * lev_rows % LANES == 0
        and lev_rows * lev_count == LANES
        and lat_count == SUB
        and modes % (2 * SUB * lat_count) == 0
        and owner_counts.shape[0] == lat_count
        and 2 * modes // lat_count % lat_count == 0
        and legendre.shape[2] <= 2 * modes
        and modes % (lat_count * lev_count) == 0
    )
    if fits:
        return on_device(lat_count, lev_count, fields, legendre, owner_counts)
    return plain_on_device(fields, legendre, owner_counts)


def solution(mesh):
    return jax.shard_map(
        functools.partial(pick, mesh.shape["lat"], mesh.shape["lev"]),
        mesh=mesh,
        in_specs=(P(None, "lev", "lat", None), P("lat", None, None), P()),
        out_specs=P("lat", "lev", None),
        check_vma=False,
    )
```

```python
import functools
import math

import jax
import jax.numpy as jnp
import numpy as np
from jax import lax
from jax.experimental import pallas as pl
from jax.experimental.pallas import tpu as pltpu
from jax.sharding import PartitionSpec as P


def fourier_table(points, modes):
    places = jnp.arange(points, dtype=jnp.int32)
    orders = jnp.arange(modes, dtype=jnp.int32)
    phase = places[:, None] * orders[None, :] % points
    angle = phase.astype(jnp.float32) * (2.0 * math.pi / points)
    factor = points ** (-0.5)
    return jnp.stack([jnp.cos(angle) * factor, -jnp.sin(angle) * factor], axis=2)


def plain_on_device(fields, legendre, owner_counts):
    members, lev_rows, lat_rows, points = fields.shape
    modes = legendre.shape[1]
    lev_count = lax.axis_size("lev")
    owners = owner_counts.shape[0]
    capacity = 2 * modes // owners
    dft_table = fourier_table(points, modes)
    spectra = jnp.einsum("belx,xmc->lmcbe", fields, dft_table, precision=lax.Precision.HIGHEST)
    spectra = spectra.reshape(lat_rows, modes, 2 * members * lev_rows).astype(jnp.bfloat16)
    collected_rows, transform_table_rows = (
        lax.all_to_all(spectra, "lat", split_axis=1, concat_axis=0, tiled=True),
        lax.all_to_all(legendre, "lat", split_axis=1, concat_axis=0, tiled=True),
    )
    wavenumber_rows = jnp.einsum(
        "dez,det->tez", collected_rows, transform_table_rows, preferred_element_type=jnp.float32
    )
    resident_modes = wavenumber_rows.shape[1]
    shaped = wavenumber_rows.reshape(modes, resident_modes, 2, members, lev_rows)
    anomaly = (shaped - jnp.mean(shaped, axis=3, keepdims=True)).astype(jnp.bfloat16)
    anomaly = anomaly.reshape(modes, resident_modes, 2 * members * lev_rows)
    starts = jnp.cumsum(owner_counts) - owner_counts
    offset = jnp.arange(capacity, dtype=jnp.int32)
    active_flag = offset[None, :] < owner_counts[:, None]
    slot_index = jnp.where(active_flag, starts[:, None] + offset[None, :], 0).reshape(-1)
    slotted = jnp.take(anomaly, slot_index, axis=0)
    slotted = jnp.where(active_flag.reshape(-1)[:, None, None], slotted, jnp.zeros_like(slotted))
    slotted = slotted[None]
    received = lax.all_to_all(
        lax.all_to_all(slotted, "lat", split_axis=1, concat_axis=2, tiled=True),
        "lev",
        split_axis=2,
        concat_axis=0,
        tiled=True,
    )
    mode_share = received.shape[2]
    blocks = received.reshape(lev_count, capacity, mode_share, 2 * members, lev_rows)
    partial_value = jnp.einsum(
        "esaql,fsaqk->selfk", blocks, blocks, preferred_element_type=jnp.float32
    )
    partial_value = partial_value.reshape(capacity, lev_count * lev_rows, lev_count * lev_rows)
    summed = lax.psum_scatter(partial_value, "lev", scatter_dimension=1, tiled=True)
    owner = lax.axis_index("lat")
    wavenumber = starts[owner] + offset
    live_count = owner_counts[owner]
    divisor = ((members - 1) * (2 * wavenumber + 2)).astype(jnp.float32)
    scaled = summed / divisor[:, None, None]
    return jnp.where((offset < live_count)[:, None, None], scaled, jnp.zeros_like(scaled))


LANES = 128
SUB = 8
VMEM_LIMIT = 67_043_328


def split_bf16(values):
    high = values.astype(jnp.bfloat16)
    return high, (values - high.astype(jnp.float32)).astype(jnp.bfloat16)


def folded_tables(points, orders):
    tables = []
    for residues, length in (((1, 3), points // 2), ((0,), points // 4), ((2,), points // 4)):
        m = orders[np.isin(orders % 4, residues)]
        angle = 2.0 * np.pi * ((m[:, None] * np.arange(length)[None, :]) % points) / points
        table = np.concatenate([np.cos(angle), -np.sin(angle)]) * points ** -0.5
        table = table.astype(np.float32)
        high = table.astype(jnp.bfloat16)
        low = (table - high.astype(np.float32)).astype(jnp.bfloat16)
        tables.append(np.stack([high, low]))
    return tables


NT = (((1,), (1,)), ((), ()))
TN = (((0,), (0,)), ((), ()))


def block_of(i, j, lat_count):
    return i * lat_count + j if i % 2 == 0 else (i + 1) * lat_count - 1 - j


def main_kernel(size, *refs):
    lat_count, lev_count, members, lev_rows, totals, counts = size
    c_ref, f_ref, g_ref, odd_ref, zero_ref, two_ref, out_ref = refs[:7]
    blocks = counts
    t_refs = refs[7:7 + blocks]
    (wide, held, sent, got, out_waves, in_waves, joined_ref) = refs[7 + blocks:14 + blocks]
    (part_out, part_in, rows_out, rows_in, slots_out, slots_in) = refs[14 + blocks:20 + blocks]
    (f_sem, own_sem, t_send, t_recv, s_send, s_recv, z_send, z_recv) = refs[20 + blocks:28 + blocks]
    (p_send, p_recv, l_send, l_recv, d_send, d_recv) = refs[28 + blocks:]
    me = lax.axis_index("lat")
    depth = lax.axis_index("lev")
    groups = members * lev_rows // LANES
    lat_rows = f_ref.shape[1] * SUB
    pieces = f_ref.shape[3] // LANES
    halves = 2
    eras = lat_rows // (SUB * halves)
    steps = eras * groups
    pairs = 2 * groups
    pack = LANES // lev_rows
    band = SUB * lev_count
    bands = totals // band
    first_band = [i * lat_count // lev_count for i in range(blocks)]
    base = []
    for i in range(blocks):
        base.append(sum(bands - first_band[b] for b in range(i)) - first_band[i])
    lows = [totals - t_refs[i].shape[-1] for i in range(blocks)]
    columns = [[(low, totals, i)] for i, low in enumerate(lows)]
    if totals - lows[0] > LANES:
        columns[0] = [(totals - LANES, totals, 0), (lows[0], totals - LANES, blocks)]

    def lat_peer(offset):
        return lax.rem(me + offset, lat_count)

    def lev_peer(offset):
        return lax.rem(depth + offset, lev_count)

    def fetch_copy(e, half, c):
        l, g = e // groups * halves + half, lax.rem(e, groups)
        return pltpu.make_async_copy(
            f_ref.at[pl.ds(pl.multiple_of(g * LANES, LANES), LANES), l, :, c * LANES:(c + 1) * LANES],
            wide.at[pl.ds((half * pieces + c) * LANES, LANES)],
            f_sem.at[half],
        )

    def fetch_start(e, half):
        for c in range(pieces):
            fetch_copy(e, half, c).start()

    def fetch_wait(half):
        span = wide.at[pl.ds(half * pieces * LANES, pieces * LANES)]
        pltpu.make_async_copy(span, span, f_sem.at[half]).wait()

    def table_source(i, target, start, stop):
        row = pl.multiple_of(block_of(i, target, lat_count) * SUB, SUB)
        return g_ref.at[:, pl.ds(row, SUB), start:stop]

    def table_send(i, part):
        start, stop, sem = part
        for offset in range(1, lat_count):
            target = lat_peer(offset)
            pltpu.make_async_remote_copy(
                src_ref=table_source(i, target, start, stop),
                dst_ref=t_refs[i].at[me, :, :, start - lows[i]:stop - lows[i]],
                send_sem=t_send.at[sem],
                recv_sem=t_recv.at[sem],
                device_id={"lat": target},
                device_id_type=pl.DeviceIdType.MESH,
            ).start()

    def own_table(i):
        return pltpu.make_async_copy(table_source(i, me, lows[i], totals), t_refs[i].at[me], own_sem.at[i])

    def own_spectra(i):
        return pltpu.make_async_copy(sent.at[me, i], got.at[i, me], own_sem.at[blocks + i])

    def spectra_send(i, e):
        for offset in range(1, lat_count):
            target = lat_peer(offset)
            pltpu.make_async_remote_copy(
                src_ref=sent.at[target, i, e],
                dst_ref=got.at[i, me, e],
                send_sem=s_send,
                recv_sem=s_recv.at[i],
                device_id={"lat": target},
                device_id_type=pl.DeviceIdType.MESH,
            ).start()

    def waves_copy(place, offset):
        target = lev_peer(offset)
        return pltpu.make_async_remote_copy(
            src_ref=out_waves.at[place, target],
            dst_ref=in_waves.at[place, depth],
            send_sem=z_send.at[place, offset - 1],
            recv_sem=z_recv.at[place],
            device_id={"lev": target},
            device_id_type=pl.DeviceIdType.MESH,
        )

    def for_waves(i, t, act):
        for offset in range(1, lev_count):

            @pl.when(t * lev_count + lev_peer(offset) >= block_of(i, me, lat_count))
            def _():
                act(waves_copy(base[i] + t, offset))

    def settle(ref, sem):
        pltpu.make_async_copy(ref, ref, sem).wait()

    for half in range(halves):
        fetch_start(0, half)
    barrier = pltpu.get_barrier_semaphore()
    for offset in range(1, lat_count):
        pl.semaphore_signal(
            barrier, inc=1, device_id={"lat": lat_peer(offset)}, device_id_type=pl.DeviceIdType.MESH
        )
    for offset in range(1, lev_count):
        pl.semaphore_signal(
            barrier, inc=1, device_id={"lev": lev_peer(offset)}, device_id_type=pl.DeviceIdType.MESH
        )
    pl.semaphore_wait(barrier, lat_count + lev_count - 2)
    table_send(0, columns[0][0])
    for i in range(blocks):
        own_table(i).start()

    rows_view = wide.reshape(wide.shape[0] * SUB, LANES)
    span = SUB * halves
    block_total = lat_count * blocks

    def transform(table_ref, values):
        high, low = split_bf16(values)
        dot = functools.partial(lax.dot_general, dimension_numbers=NT, preferred_element_type=jnp.float32)
        count = table_ref.shape[1]
        both = dot(table_ref[...].reshape(2 * count, table_ref.shape[2]), high)
        return both[:count] + (both[count:] + dot(table_ref[0], low))

    quarter = pieces * LANES // 4
    kinds = [[r for r in range(SUB) if r % 4 in k] for k in ((1, 3), (0,), (2,))]
    kind_rows = [2 * block_total * sum(len(k) for k in kinds[:n]) for n in range(len(kinds))]

    def spectra_step(e, carry):
        for half in range(halves):
            fetch_wait(half)

            def pair_step(pair, carry):
                lat = 2 * pair
                values = [
                    jnp.concatenate(
                        [
                            rows_view[pl.ds((half * pieces + c) * LANES * SUB + lat + s, LANES, SUB), :]
                            for s in range(2)
                        ],
                        axis=0,
                    )
                    for c in range(pieces)
                ]
                middle = pieces // 2
                even = jnp.concatenate([u + v for u, v in zip(values[:middle], values[middle:])], axis=1)
                odd = jnp.concatenate([u - v for u, v in zip(values[:middle], values[middle:])], axis=1)
                parts = (
                    transform(odd_ref, odd),
                    transform(zero_ref, even[:, :quarter] + even[:, quarter:]),
                    transform(two_ref, even[:, :quarter] - even[:, quarter:]),
                )
                for s in range(2):
                    for row, sums in zip(kind_rows, parts):
                        held[half, pl.ds(row * SUB + lat + s, sums.shape[0], SUB), :] = (
                            sums[:, s * LANES:(s + 1) * LANES]
                        )
                return carry

            lax.fori_loop(0, SUB // 2, pair_step, 0)

            @pl.when(e < steps - 1)
            def _():
                fetch_start(e + 1, half)

        def emit(target, carry):
            for i in range(blocks):
                for first, kind in zip(kind_rows, kinds):
                    for n, order in enumerate(kind):
                        for q in range(2):
                            row = first + (q * len(kind) + n) * block_total + target * blocks + i
                            rows = pl.ds(pl.multiple_of(row * SUB, SUB), SUB)
                            block = jnp.concatenate([held[half, rows, :] for half in range(halves)], axis=0)
                            sent[target, i, e, order, :, q * LANES:(q + 1) * LANES] = block.astype(jnp.bfloat16)
            return carry

        lax.fori_loop(0, lat_count, emit, 0)
        spectra_send(0, e)
        return carry

    lax.fori_loop(0, steps, spectra_step, 0)
    for i in range(blocks):
        own_spectra(i).start()
    for part in columns[0][1:]:
        table_send(0, part)
    for i in range(1, blocks):
        for part in columns[i]:
            table_send(i, part)

        def rest(e, carry):
            spectra_send(i, e)
            return carry

        lax.fori_loop(0, steps, rest, 0)

    cov = held.reshape(2 * held.shape[1], LANES)

    def cov_rows(r, t):
        return pl.ds(pl.multiple_of((r * bands + t) * LANES, LANES), LANES)

    def zero(n, carry):
        cov[cov_rows(0, n), :] = jnp.zeros((LANES, LANES), jnp.float32)
        return carry

    lax.fori_loop(0, SUB * bands, zero, 0)

    depth_rows = lat_count * lat_rows
    table_base = pairs * totals * SUB

    def legendre_sum(i):
        own_table(i).wait()
        for n, part in enumerate(columns[i]):
            legendre_part(i, part, n == 0)

    def legendre_part(i, part, first):
        left, right, sem = part
        width = right - left
        low = left - lows[i]
        settle(t_refs[i].at[pl.ds(0, lat_count - 1), :, :, low:low + width], t_recv.at[sem])

        def spread(source, carry):
            for w in range(width // LANES):
                for era in range(eras):
                    at = table_base // SUB + w * depth_rows + (era * lat_count + source) * span
                    wide[pl.ds(at, span)] = t_refs[i][
                        source, era * span:(era + 1) * span, :, low + w * LANES:low + (w + 1) * LANES
                    ].astype(jnp.float32)
            return carry

        lax.fori_loop(0, lat_count, spread, 0)
        if first:
            own_spectra(i).wait()
            settle(got.at[i, pl.ds(0, lat_count - 1)], s_recv.at[i])
        skip = max(first_band[i] * band - left, 0)
        place_row = (left + skip - first_band[i] * band) * SUB

        def one(m, carry):
            table = jnp.concatenate(
                [
                    rows_view[pl.ds(table_base + w * depth_rows * SUB + m, depth_rows, SUB), :]
                    for w in range(width // LANES)
                ],
                axis=1,
            ).astype(jnp.bfloat16)
            waves = []
            for g in range(groups):
                x = jnp.concatenate(
                    [got[i, :, era * groups + g, m].reshape(lat_count * span, 2 * LANES) for era in range(eras)],
                    axis=0,
                )
                full = lax.dot_general(table, x, TN, preferred_element_type=jnp.float32)
                waves.append(full[skip:])
            for q in range(2):
                parts = [w[:, q * LANES:(q + 1) * LANES] for w in waves]
                total = functools.reduce(jnp.add, parts)
                shift = LANES // 2
                while shift >= lev_rows:
                    total = total + pltpu.roll(total, shift, 1)
                    shift //= 2
                mean = total * (1.0 / members)
                for g in range(groups):
                    rows = pl.ds((2 * g + q) * totals * SUB + place_row + m, parts[g].shape[0], SUB)
                    rows_view[rows, :] = parts[g] - mean
            return carry

        lax.fori_loop(0, SUB, one, 0)
        start = jnp.maximum(block_of(i, me, lat_count) // lev_count, left // band)

        def emit(t, carry):
            place = base[i] + t
            for w in range(pairs):
                for z in range(lev_count):
                    row = w * totals * SUB + ((t - first_band[i]) * lev_count + z) * SUB * SUB
                    block = rows_view[pl.ds(pl.multiple_of(row, SUB), SUB * SUB), :].astype(jnp.bfloat16)
                    out_waves[place, z, :, w * LANES:(w + 1) * LANES] = block
            for_waves(i, t, lambda copy: copy.start())
            in_waves[place, depth] = out_waves[place, depth]
            return carry

        lax.fori_loop(start, right // band, emit, 0)

    def covariance(i, low, high):
        start = (block_of(i, me, lat_count) + lev_count - 1 - depth) // lev_count

        def one(t, carry):
            place = base[i] + t
            settle(in_waves.at[place, pl.ds(0, lev_count - 1)], z_recv.at[place])
            for w in range(pairs):
                parts = [
                    in_waves[place, v, :, w * LANES:(w + 1) * LANES].astype(jnp.float32)
                    for v in range(lev_count)
                ]
                for s in range(pack):
                    joined = jnp.concatenate([p[:, s * lev_rows:(s + 1) * lev_rows] for p in parts], axis=1)
                    joined_ref[:, w * pack + s] = joined.reshape(SUB, SUB, LANES)

            def multiply(n, carry):
                for s in range(SUB // 2):
                    r = n * (SUB // 2) + s
                    x = joined_ref[r].reshape(pairs * pack * SUB, LANES).astype(jnp.bfloat16)
                    cov[cov_rows(r, t), :] += lax.dot_general(x, x, TN, preferred_element_type=jnp.float32)
                return carry

            lax.fori_loop(0, 2, multiply, 0)
            return carry

        lax.fori_loop(jnp.maximum(start, low), high, one, 0)

    def partials(low, high):
        def one(t, carry):
            for r in range(lat_count):
                part_out[t, r] = cov[cov_rows(r, t), :].astype(jnp.bfloat16)
            for offset in range(1, lat_count):
                target = lat_peer(offset)
                pltpu.make_async_remote_copy(
                    src_ref=part_out.at[t, target],
                    dst_ref=part_in.at[t, me],
                    send_sem=p_send,
                    recv_sem=p_recv.at[t],
                    device_id={"lat": target},
                    device_id_type=pl.DeviceIdType.MESH,
                ).start()
            part_in[t, me] = part_out[t, me]
            return carry

        lax.fori_loop(low, high, one, 0)

    def totals_over_lat(low, high):
        def one(t, carry):
            settle(part_in.at[t, pl.ds(0, lat_count - 1)], p_recv.at[t])
            for z in range(lev_count):
                rows = slice(z * lev_rows, (z + 1) * lev_rows)
                total = part_in[t, 0, rows].astype(jnp.float32)
                for source in range(1, lat_count):
                    total = total + part_in[t, source, rows].astype(jnp.float32)
                rows_out[z, t] = total.astype(jnp.bfloat16)
            for offset in range(1, lev_count):
                target = lev_peer(offset)
                pltpu.make_async_remote_copy(
                    src_ref=rows_out.at[target, t],
                    dst_ref=rows_in.at[depth, t],
                    send_sem=l_send,
                    recv_sem=l_recv,
                    device_id={"lev": target},
                    device_id_type=pl.DeviceIdType.MESH,
                ).start()
            rows_in[depth, t] = rows_out[depth, t]
            return carry

        lax.fori_loop(low, high, one, 0)

    for i in range(blocks):
        legendre_sum(i)
        if i > 0 and i < blocks - 1:
            covariance(i - 1, 0, bands)
            partials(first_band[i - 1], first_band[i])
    covariance(blocks - 2, 0, bands)
    partials(first_band[blocks - 2], first_band[blocks - 1])
    for t in range(first_band[blocks - 1], bands):
        covariance(blocks - 1, t, t + 1)
        partials(t, t + 1)
    early = first_band[blocks // 2]
    totals_over_lat(0, early)
    totals_over_lat(early, bands)
    settle(rows_in.at[pl.ds(0, lev_count - 1)], l_recv)

    share = slots_out.shape[1]
    start, mine, count = 0, 0, 0
    for d in range(lat_count):
        held_here = c_ref[d]
        mine = jnp.where(d == me, start, mine)
        count = jnp.where(d == me, held_here, count)
        first = start // lat_count + jnp.where(start % lat_count > me, 1, 0)
        for k in range(share):
            rank = jnp.minimum(first + k, bands * lev_count - 1)
            slots_out[d, k] = rows_in[rank % lev_count, rank // lev_count]
        start = start + held_here
    for offset in range(1, lat_count):
        target = lat_peer(offset)
        pltpu.make_async_remote_copy(
            src_ref=slots_out.at[target],
            dst_ref=slots_in.at[me],
            send_sem=d_send,
            recv_sem=d_recv,
            device_id={"lat": target},
            device_id_type=pl.DeviceIdType.MESH,
        ).start()
    slots_in[me] = slots_out[me]
    settle(slots_in.at[pl.ds(0, lat_count - 1)], d_recv)

    def finish(k, carry):
        for o in range(lat_count):
            offset = k * lat_count + o
            wavenumber = mine + offset
            divisor = ((members - 1) * (2 * wavenumber + 2)).astype(jnp.float32)
            chosen = slots_in[wavenumber % lat_count, k].astype(jnp.float32) / divisor
            out_ref[offset] = jnp.where(offset < count, chosen, jnp.zeros_like(chosen))
        return carry

    lax.fori_loop(0, share, finish, 0)
    settle(part_out.at[:, pl.ds(0, lat_count - 1)], p_send)
    settle(rows_out.at[pl.ds(0, lev_count - 1)], l_send)
    settle(slots_out.at[pl.ds(0, lat_count - 1)], d_send)
    settle(sent.at[pl.ds(0, lat_count - 1)], s_send)
    for i in range(blocks):
        for left, right, sem in columns[i]:
            part = t_refs[i].at[pl.ds(0, lat_count - 1), :, :, left - lows[i]:right - lows[i]]
            settle(part, t_send.at[sem])

        def drain(t, carry):
            for_waves(i, t, lambda copy: copy.wait_send())
            return carry

        lax.fori_loop(block_of(i, me, lat_count) // lev_count, bands, drain, 0)


def on_device(lat_count, lev_count, fields, legendre, owner_counts):
    members, lev_rows, lat_rows, points = fields.shape
    modes, totals = legendre.shape[1:]
    rows = members * lev_rows
    groups = rows // LANES
    blocks = modes // (SUB * lat_count)
    bands = totals // (SUB * lev_count)
    levels = lev_count * lev_rows
    span = 2 * SUB
    steps = lat_rows // span * groups
    starts = [block_of(i, j, lat_count) * SUB for j in range(lat_count) for i in range(blocks)]
    orders = np.concatenate([np.array(starts) + r for r in range(SUB)])
    tables = [jnp.asarray(t) for t in folded_tables(points, orders)]
    places = sum(bands - i * lat_count // lev_count for i in range(blocks))
    widths = [totals - i * lat_count * SUB // LANES * LANES for i in range(blocks)]
    wide = max(2 * points, 2 * groups * totals + totals // LANES * lat_count * lat_rows)
    size = (lat_count, lev_count, members, lev_rows, totals, blocks)
    vmem = pl.BlockSpec(memory_space=pltpu.VMEM)
    hbm = pl.BlockSpec(memory_space=pl.ANY)
    smem = pl.BlockSpec(memory_space=pltpu.SMEM)
    capacity = 2 * modes // owner_counts.shape[0]
    share = capacity // lat_count
    return pl.pallas_call(
        functools.partial(main_kernel, size),
        out_shape=jax.ShapeDtypeStruct((capacity, lev_rows, levels), jnp.float32),
        in_specs=[smem, hbm, hbm, vmem, vmem, vmem],
        out_specs=vmem,
        scratch_shapes=[pltpu.VMEM((lat_count, lat_rows, SUB, w), jnp.bfloat16) for w in widths]
        + [
            pltpu.VMEM((wide, SUB, LANES), jnp.float32),
            pltpu.VMEM((2, modes * span, LANES), jnp.float32),
            pltpu.VMEM((lat_count, blocks, steps, SUB, span, 2 * LANES), jnp.bfloat16),
            pltpu.VMEM((blocks, lat_count, steps, SUB, span, 2 * LANES), jnp.bfloat16),
            pltpu.VMEM((places, lev_count, SUB * SUB, 2 * rows), jnp.bfloat16),
            pltpu.VMEM((places, lev_count, SUB * SUB, 2 * rows), jnp.bfloat16),
            pltpu.VMEM((SUB, 2 * groups * (LANES // lev_rows), SUB, LANES), jnp.float32),
            pltpu.VMEM((bands, lat_count, levels, levels), jnp.bfloat16),
            pltpu.VMEM((bands, lat_count, levels, levels), jnp.bfloat16),
            pltpu.VMEM((lev_count, bands, lev_rows, levels), jnp.bfloat16),
            pltpu.VMEM((lev_count, bands, lev_rows, levels), jnp.bfloat16),
            pltpu.VMEM((lat_count, share, lev_rows, levels), jnp.bfloat16),
            pltpu.VMEM((lat_count, share, lev_rows, levels), jnp.bfloat16),
            pltpu.SemaphoreType.DMA((2,)),
            pltpu.SemaphoreType.DMA((2 * blocks,)),
            pltpu.SemaphoreType.DMA((blocks + 1,)),
            pltpu.SemaphoreType.DMA((blocks + 1,)),
            pltpu.SemaphoreType.DMA,
            pltpu.SemaphoreType.DMA((blocks,)),
            pltpu.SemaphoreType.DMA((places, lev_count - 1)),
            pltpu.SemaphoreType.DMA((places,)),
            pltpu.SemaphoreType.DMA,
            pltpu.SemaphoreType.DMA((bands,)),
            pltpu.SemaphoreType.DMA,
            pltpu.SemaphoreType.DMA,
            pltpu.SemaphoreType.DMA,
            pltpu.SemaphoreType.DMA,
        ],
        compiler_params=pltpu.CompilerParams(
            vmem_limit_bytes=VMEM_LIMIT, collective_id=0, has_side_effects=True
        ),
        cost_estimate=pl.CostEstimate(flops=40_000_000_000, bytes_accessed=80_000_000, transcendentals=0),
    )(owner_counts, fields.reshape(rows, lat_rows // SUB, SUB, points), legendre, *tables)


def pick(lat_count, lev_count, fields, legendre, owner_counts):
    members, lev_rows, lat_rows, points = fields.shape
    modes = legendre.shape[1]
    fits = (
        lat_rows % 16 == 0
        and members * lev_rows % LANES == 0
        and lev_rows * lev_count == LANES
        and lat_count == SUB
        and modes % (2 * SUB * lat_count) == 0
        and owner_counts.shape[0] == lat_count
        and 2 * modes // lat_count % lat_count == 0
        and legendre.shape[2] <= 2 * modes
        and modes % (lat_count * lev_count) == 0
    )
    if fits:
        return on_device(lat_count, lev_count, fields, legendre, owner_counts)
    return plain_on_device(fields, legendre, owner_counts)


def solution(mesh):
    return jax.shard_map(
        functools.partial(pick, mesh.shape["lat"], mesh.shape["lev"]),
        mesh=mesh,
        in_specs=(P(None, "lev", "lat", None), P("lat", None, None), P()),
        out_specs=P("lat", "lev", None),
        check_vma=False,
    )
```

```python
import functools
import math

import jax
import jax.numpy as jnp
import numpy as np
from jax import lax
from jax.experimental import pallas as pl
from jax.experimental.pallas import tpu as pltpu
from jax.sharding import PartitionSpec as P


def fourier_table(points, modes):
    places = jnp.arange(points, dtype=jnp.int32)
    orders = jnp.arange(modes, dtype=jnp.int32)
    phase = places[:, None] * orders[None, :] % points
    angle = phase.astype(jnp.float32) * (2.0 * math.pi / points)
    factor = points ** (-0.5)
    return jnp.stack([jnp.cos(angle) * factor, -jnp.sin(angle) * factor], axis=2)


def plain_on_device(fields, legendre, owner_counts):
    members, lev_rows, lat_rows, points = fields.shape
    modes = legendre.shape[1]
    lev_count = lax.axis_size("lev")
    owners = owner_counts.shape[0]
    capacity = 2 * modes // owners
    dft_table = fourier_table(points, modes)
    spectra = jnp.einsum("belx,xmc->lmcbe", fields, dft_table, precision=lax.Precision.HIGHEST)
    spectra = spectra.reshape(lat_rows, modes, 2 * members * lev_rows).astype(jnp.bfloat16)
    collected_rows, transform_table_rows = (
        lax.all_to_all(spectra, "lat", split_axis=1, concat_axis=0, tiled=True),
        lax.all_to_all(legendre, "lat", split_axis=1, concat_axis=0, tiled=True),
    )
    wavenumber_rows = jnp.einsum(
        "dez,det->tez", collected_rows, transform_table_rows, preferred_element_type=jnp.float32
    )
    resident_modes = wavenumber_rows.shape[1]
    shaped = wavenumber_rows.reshape(modes, resident_modes, 2, members, lev_rows)
    anomaly = (shaped - jnp.mean(shaped, axis=3, keepdims=True)).astype(jnp.bfloat16)
    anomaly = anomaly.reshape(modes, resident_modes, 2 * members * lev_rows)
    starts = jnp.cumsum(owner_counts) - owner_counts
    offset = jnp.arange(capacity, dtype=jnp.int32)
    active_flag = offset[None, :] < owner_counts[:, None]
    slot_index = jnp.where(active_flag, starts[:, None] + offset[None, :], 0).reshape(-1)
    slotted = jnp.take(anomaly, slot_index, axis=0)
    slotted = jnp.where(active_flag.reshape(-1)[:, None, None], slotted, jnp.zeros_like(slotted))
    slotted = slotted[None]
    received = lax.all_to_all(
        lax.all_to_all(slotted, "lat", split_axis=1, concat_axis=2, tiled=True),
        "lev",
        split_axis=2,
        concat_axis=0,
        tiled=True,
    )
    mode_share = received.shape[2]
    blocks = received.reshape(lev_count, capacity, mode_share, 2 * members, lev_rows)
    partial_value = jnp.einsum(
        "esaql,fsaqk->selfk", blocks, blocks, preferred_element_type=jnp.float32
    )
    partial_value = partial_value.reshape(capacity, lev_count * lev_rows, lev_count * lev_rows)
    summed = lax.psum_scatter(partial_value, "lev", scatter_dimension=1, tiled=True)
    owner = lax.axis_index("lat")
    wavenumber = starts[owner] + offset
    live_count = owner_counts[owner]
    divisor = ((members - 1) * (2 * wavenumber + 2)).astype(jnp.float32)
    scaled = summed / divisor[:, None, None]
    return jnp.where((offset < live_count)[:, None, None], scaled, jnp.zeros_like(scaled))


LANES = 128
SUB = 8
VMEM_LIMIT = 67_043_328


def split_bf16(values):
    high = values.astype(jnp.bfloat16)
    return high, (values - high.astype(jnp.float32)).astype(jnp.bfloat16)


def folded_tables(points, orders):
    tables = []
    for residues, length in (((1, 3), points // 2), ((0,), points // 4), ((2,), points // 4)):
        m = orders[np.isin(orders % 4, residues)]
        angle = 2.0 * np.pi * ((m[:, None] * np.arange(length)[None, :]) % points) / points
        table = np.concatenate([np.cos(angle), -np.sin(angle)]) * points ** -0.5
        table = table.astype(np.float32)
        high = table.astype(jnp.bfloat16)
        low = (table - high.astype(np.float32)).astype(jnp.bfloat16)
        tables.append(np.stack([high, low]))
    return tables


NT = (((1,), (1,)), ((), ()))
TN = (((0,), (0,)), ((), ()))


def block_of(i, j, lat_count):
    return i * lat_count + j if i % 2 == 0 else (i + 1) * lat_count - 1 - j


def main_kernel(size, *refs):
    lat_count, lev_count, members, lev_rows, totals, counts = size
    c_ref, f_ref, g_ref, odd_ref, zero_ref, two_ref, out_ref = refs[:7]
    blocks = counts
    t_refs = refs[7:7 + blocks]
    (wide, held, sent, got, out_waves, in_waves, joined_ref) = refs[7 + blocks:14 + blocks]
    (part_out, part_in, rows_out, rows_in, slots_out, slots_in) = refs[14 + blocks:20 + blocks]
    (f_sem, own_sem, t_send, t_recv, s_send, s_recv, z_send, z_recv) = refs[20 + blocks:28 + blocks]
    (p_send, p_recv, l_send, l_recv, d_send, d_recv, w_send, w_recv) = refs[28 + blocks:]
    me = lax.axis_index("lat")
    depth = lax.axis_index("lev")
    groups = members * lev_rows // LANES
    lat_rows = f_ref.shape[1] * SUB
    pieces = f_ref.shape[3] // LANES
    halves = 2
    eras = lat_rows // (SUB * halves)
    steps = eras * groups
    pairs = 2 * groups
    pack = LANES // lev_rows
    band = SUB * lev_count
    bands = totals // band
    first_band = [i * lat_count // lev_count for i in range(blocks)]
    base = []
    for i in range(blocks):
        base.append(sum(bands - first_band[b] for b in range(i)) - first_band[i])
    lows = [totals - t_refs[i].shape[-1] for i in range(blocks)]
    columns = [[(low, totals, i)] for i, low in enumerate(lows)]
    if totals - lows[0] > LANES:
        columns[0] = [(totals - LANES, totals, 0), (lows[0], totals - LANES, blocks)]
    shared = (1, blocks)
    portion = lat_rows // lev_count

    def lat_peer(offset):
        return lax.rem(me + offset, lat_count)

    def lev_peer(offset):
        return lax.rem(depth + offset, lev_count)

    def fetch_copy(e, half, c):
        l, g = e // groups * halves + half, lax.rem(e, groups)
        return pltpu.make_async_copy(
            f_ref.at[pl.ds(pl.multiple_of(g * LANES, LANES), LANES), l, :, c * LANES:(c + 1) * LANES],
            wide.at[pl.ds((half * pieces + c) * LANES, LANES)],
            f_sem.at[half],
        )

    def fetch_start(e, half):
        for c in range(pieces):
            fetch_copy(e, half, c).start()

    def fetch_wait(half):
        span = wide.at[pl.ds(half * pieces * LANES, pieces * LANES)]
        pltpu.make_async_copy(span, span, f_sem.at[half]).wait()

    def table_span(i, part):
        return slice(part[0] - lows[i], part[1] - lows[i])

    def lats_of(part):
        return pl.ds(depth * portion, portion) if part[2] in shared else pl.ds(0, lat_rows)

    def table_source(i, target, part):
        row = pl.multiple_of(block_of(i, target, lat_count) * SUB, SUB)
        return g_ref.at[lats_of(part), pl.ds(row, SUB), part[0]:part[1]]

    def table_target(i, part):
        return t_refs[i].at[me, lats_of(part), :, table_span(i, part)]

    def table_send(i, part):
        for offset in range(1, lat_count):
            target = lat_peer(offset)
            pltpu.make_async_remote_copy(
                src_ref=table_source(i, target, part),
                dst_ref=table_target(i, part),
                send_sem=t_send.at[part[2]],
                recv_sem=t_recv.at[part[2]],
                device_id={"lat": target},
                device_id_type=pl.DeviceIdType.MESH,
            ).start()

    def own_table(i, part):
        return pltpu.make_async_copy(table_source(i, me, part), table_target(i, part), own_sem.at[part[2]])

    def table_remote(i, part):
        count = portion if part[2] in shared else lat_rows
        return t_refs[i].at[pl.ds(0, lat_count - 1), pl.ds(0, count), :, table_span(i, part)]

    def table_passed(i, part):
        return t_refs[i].at[:, pl.ds(0, (lev_count - 1) * portion), :, table_span(i, part)]

    def table_arrive(i, part):
        own_table(i, part).wait()
        settle(table_remote(i, part), t_recv.at[part[2]])

    def table_pass(i, part):
        table_arrive(i, part)
        block = t_refs[i].at[:, lats_of(part), :, table_span(i, part)]
        for offset in range(1, lev_count):
            pltpu.make_async_remote_copy(
                src_ref=block,
                dst_ref=block,
                send_sem=w_send.at[part[2]],
                recv_sem=w_recv.at[part[2]],
                device_id={"lev": lev_peer(offset)},
                device_id_type=pl.DeviceIdType.MESH,
            ).start()

    def shared_parts():
        return [(i, part) for i in range(blocks) for part in columns[i] if part[2] in shared]

    def own_spectra(i):
        return pltpu.make_async_copy(sent.at[me, i], got.at[i, me], own_sem.at[blocks + 1 + i])

    def spectra_send(i, e):
        for offset in range(1, lat_count):
            target = lat_peer(offset)
            pltpu.make_async_remote_copy(
                src_ref=sent.at[target, i, e],
                dst_ref=got.at[i, me, e],
                send_sem=s_send,
                recv_sem=s_recv.at[i],
                device_id={"lat": target},
                device_id_type=pl.DeviceIdType.MESH,
            ).start()

    def waves_copy(place, offset):
        target = lev_peer(offset)
        return pltpu.make_async_remote_copy(
            src_ref=out_waves.at[place, target],
            dst_ref=in_waves.at[place, depth],
            send_sem=z_send.at[place, offset - 1],
            recv_sem=z_recv.at[place],
            device_id={"lev": target},
            device_id_type=pl.DeviceIdType.MESH,
        )

    def for_waves(i, t, act):
        for offset in range(1, lev_count):

            @pl.when(t * lev_count + lev_peer(offset) >= block_of(i, me, lat_count))
            def _():
                act(waves_copy(base[i] + t, offset))

    def settle(ref, sem):
        pltpu.make_async_copy(ref, ref, sem).wait()

    for half in range(halves):
        fetch_start(0, half)
    barrier = pltpu.get_barrier_semaphore()
    for offset in range(1, lat_count):
        pl.semaphore_signal(
            barrier, inc=1, device_id={"lat": lat_peer(offset)}, device_id_type=pl.DeviceIdType.MESH
        )
    for offset in range(1, lev_count):
        pl.semaphore_signal(
            barrier, inc=1, device_id={"lev": lev_peer(offset)}, device_id_type=pl.DeviceIdType.MESH
        )
    pl.semaphore_wait(barrier, lat_count + lev_count - 2)
    table_send(0, columns[0][0])
    for i, part in shared_parts():
        table_send(i, part)
    for i in range(blocks):
        for part in columns[i]:
            own_table(i, part).start()

    rows_view = wide.reshape(wide.shape[0] * SUB, LANES)
    span = SUB * halves
    block_total = lat_count * blocks

    def transform(table_ref, values):
        high, low = split_bf16(values)
        dot = functools.partial(lax.dot_general, dimension_numbers=NT, preferred_element_type=jnp.float32)
        count = table_ref.shape[1]
        both = dot(table_ref[...].reshape(2 * count, table_ref.shape[2]), high)
        return both[:count] + (both[count:] + dot(table_ref[0], low))

    quarter = pieces * LANES // 4
    kinds = [[r for r in range(SUB) if r % 4 in k] for k in ((1, 3), (0,), (2,))]
    kind_rows = [2 * block_total * sum(len(k) for k in kinds[:n]) for n in range(len(kinds))]

    def spectra_step(e, carry):
        for half in range(halves):
            fetch_wait(half)

            def pair_step(pair, carry):
                lat = 2 * pair
                values = [
                    jnp.concatenate(
                        [
                            rows_view[pl.ds((half * pieces + c) * LANES * SUB + lat + s, LANES, SUB), :]
                            for s in range(2)
                        ],
                        axis=0,
                    )
                    for c in range(pieces)
                ]
                middle = pieces // 2
                even = jnp.concatenate([u + v for u, v in zip(values[:middle], values[middle:])], axis=1)
                odd = jnp.concatenate([u - v for u, v in zip(values[:middle], values[middle:])], axis=1)
                parts = (
                    transform(odd_ref, odd),
                    transform(zero_ref, even[:, :quarter] + even[:, quarter:]),
                    transform(two_ref, even[:, :quarter] - even[:, quarter:]),
                )
                for s in range(2):
                    for row, sums in zip(kind_rows, parts):
                        held[half, pl.ds(row * SUB + lat + s, sums.shape[0], SUB), :] = (
                            sums[:, s * LANES:(s + 1) * LANES]
                        )
                return carry

            lax.fori_loop(0, SUB // 2, pair_step, 0)

            @pl.when(e < steps - 1)
            def _():
                fetch_start(e + 1, half)

        def emit(target, carry):
            for i in range(blocks):
                for first, kind in zip(kind_rows, kinds):
                    for n, order in enumerate(kind):
                        for q in range(2):
                            row = first + (q * len(kind) + n) * block_total + target * blocks + i
                            rows = pl.ds(pl.multiple_of(row * SUB, SUB), SUB)
                            block = jnp.concatenate([held[half, rows, :] for half in range(halves)], axis=0)
                            sent[target, i, e, order, :, q * LANES:(q + 1) * LANES] = block.astype(jnp.bfloat16)
            return carry

        lax.fori_loop(0, lat_count, emit, 0)
        spectra_send(0, e)

        @pl.when(e == steps // 2 - 1)
        def _():
            for i, part in shared_parts():
                table_pass(i, part)

        return carry

    lax.fori_loop(0, steps, spectra_step, 0)
    for i in range(blocks):
        own_spectra(i).start()
    for i in range(1, blocks):
        for part in columns[i]:
            if part[2] not in shared:
                table_send(i, part)

        def rest(e, carry):
            spectra_send(i, e)
            return carry

        lax.fori_loop(0, steps, rest, 0)

    cov = held.reshape(2 * held.shape[1], LANES)

    def cov_rows(r, t):
        return pl.ds(pl.multiple_of((r * bands + t) * LANES, LANES), LANES)

    def zero(n, carry):
        cov[cov_rows(0, n), :] = jnp.zeros((LANES, LANES), jnp.float32)
        return carry

    lax.fori_loop(0, SUB * bands, zero, 0)

    depth_rows = lat_count * lat_rows
    table_base = pairs * totals * SUB

    def legendre_sum(i):
        for n, part in enumerate(columns[i]):
            legendre_part(i, part, n == 0)

    def legendre_part(i, part, first):
        left, right, sem = part
        width = right - left
        low = left - lows[i]
        if sem in shared:
            settle(table_passed(i, part), w_recv.at[sem])
        else:
            table_arrive(i, part)

        def spread(source, carry):
            for w in range(width // LANES):
                for era in range(eras):
                    at = table_base // SUB + w * depth_rows + (era * lat_count + source) * span
                    wide[pl.ds(at, span)] = t_refs[i][
                        source, era * span:(era + 1) * span, :, low + w * LANES:low + (w + 1) * LANES
                    ].astype(jnp.float32)
            return carry

        lax.fori_loop(0, lat_count, spread, 0)
        if first:
            own_spectra(i).wait()
            settle(got.at[i, pl.ds(0, lat_count - 1)], s_recv.at[i])
        skip = max(first_band[i] * band - left, 0)
        place_row = (left + skip - first_band[i] * band) * SUB

        def one(m, carry):
            table = jnp.concatenate(
                [
                    rows_view[pl.ds(table_base + w * depth_rows * SUB + m, depth_rows, SUB), :]
                    for w in range(width // LANES)
                ],
                axis=1,
            ).astype(jnp.bfloat16)
            waves = []
            for g in range(groups):
                x = jnp.concatenate(
                    [got[i, :, era * groups + g, m].reshape(lat_count * span, 2 * LANES) for era in range(eras)],
                    axis=0,
                )
                full = lax.dot_general(table, x, TN, preferred_element_type=jnp.float32)
                waves.append(full[skip:])
            for q in range(2):
                parts = [w[:, q * LANES:(q + 1) * LANES] for w in waves]
                total = functools.reduce(jnp.add, parts)
                shift = LANES // 2
                while shift >= lev_rows:
                    total = total + pltpu.roll(total, shift, 1)
                    shift //= 2
                mean = total * (1.0 / members)
                for g in range(groups):
                    rows = pl.ds((2 * g + q) * totals * SUB + place_row + m, parts[g].shape[0], SUB)
                    rows_view[rows, :] = parts[g] - mean
            return carry

        lax.fori_loop(0, SUB, one, 0)
        start = jnp.maximum(block_of(i, me, lat_count) // lev_count, left // band)

        def emit(t, carry):
            place = base[i] + t
            for w in range(pairs):
                for z in range(lev_count):
                    row = w * totals * SUB + ((t - first_band[i]) * lev_count + z) * SUB * SUB
                    block = rows_view[pl.ds(pl.multiple_of(row, SUB), SUB * SUB), :].astype(jnp.bfloat16)
                    out_waves[place, z, :, w * LANES:(w + 1) * LANES] = block
            for_waves(i, t, lambda copy: copy.start())
            in_waves[place, depth] = out_waves[place, depth]
            return carry

        lax.fori_loop(start, right // band, emit, 0)

    def covariance(i, low, high):
        start = (block_of(i, me, lat_count) + lev_count - 1 - depth) // lev_count

        def one(t, carry):
            place = base[i] + t
            settle(in_waves.at[place, pl.ds(0, lev_count - 1)], z_recv.at[place])
            for w in range(pairs):
                parts = [
                    in_waves[place, v, :, w * LANES:(w + 1) * LANES].astype(jnp.float32)
                    for v in range(lev_count)
                ]
                for s in range(pack):
                    joined = jnp.concatenate([p[:, s * lev_rows:(s + 1) * lev_rows] for p in parts], axis=1)
                    joined_ref[:, w * pack + s] = joined.reshape(SUB, SUB, LANES)

            def multiply(n, carry):
                for s in range(SUB // 2):
                    r = n * (SUB // 2) + s
                    x = joined_ref[r].reshape(pairs * pack * SUB, LANES).astype(jnp.bfloat16)
                    cov[cov_rows(r, t), :] += lax.dot_general(x, x, TN, preferred_element_type=jnp.float32)
                return carry

            lax.fori_loop(0, 2, multiply, 0)
            return carry

        lax.fori_loop(jnp.maximum(start, low), high, one, 0)

    def partials(low, high):
        def one(t, carry):
            for r in range(lat_count):
                part_out[t, r] = cov[cov_rows(r, t), :].astype(jnp.bfloat16)
            for offset in range(1, lat_count):
                target = lat_peer(offset)
                pltpu.make_async_remote_copy(
                    src_ref=part_out.at[t, target],
                    dst_ref=part_in.at[t, me],
                    send_sem=p_send,
                    recv_sem=p_recv.at[t],
                    device_id={"lat": target},
                    device_id_type=pl.DeviceIdType.MESH,
                ).start()
            part_in[t, me] = part_out[t, me]
            return carry

        lax.fori_loop(low, high, one, 0)

    def totals_over_lat(low, high):
        def one(t, carry):
            settle(part_in.at[t, pl.ds(0, lat_count - 1)], p_recv.at[t])
            for z in range(lev_count):
                rows = slice(z * lev_rows, (z + 1) * lev_rows)
                total = part_in[t, 0, rows].astype(jnp.float32)
                for source in range(1, lat_count):
                    total = total + part_in[t, source, rows].astype(jnp.float32)
                rows_out[z, t] = total.astype(jnp.bfloat16)
            for offset in range(1, lev_count):
                target = lev_peer(offset)
                pltpu.make_async_remote_copy(
                    src_ref=rows_out.at[target, t],
                    dst_ref=rows_in.at[depth, t],
                    send_sem=l_send,
                    recv_sem=l_recv,
                    device_id={"lev": target},
                    device_id_type=pl.DeviceIdType.MESH,
                ).start()
            rows_in[depth, t] = rows_out[depth, t]
            return carry

        lax.fori_loop(low, high, one, 0)

    for i in range(blocks):
        legendre_sum(i)
        if i > 0 and i < blocks - 1:
            covariance(i - 1, 0, bands)
            partials(first_band[i - 1], first_band[i])
    covariance(blocks - 2, 0, bands)
    partials(first_band[blocks - 2], first_band[blocks - 1])
    for t in range(first_band[blocks - 1], bands):
        covariance(blocks - 1, t, t + 1)
        partials(t, t + 1)
    early = first_band[blocks // 2]
    totals_over_lat(0, early)
    totals_over_lat(early, bands)
    settle(rows_in.at[pl.ds(0, lev_count - 1)], l_recv)

    share = slots_out.shape[1]
    start, mine, count = 0, 0, 0
    for d in range(lat_count):
        held_here = c_ref[d]
        mine = jnp.where(d == me, start, mine)
        count = jnp.where(d == me, held_here, count)
        first = start // lat_count + jnp.where(start % lat_count > me, 1, 0)
        for k in range(share):
            rank = jnp.minimum(first + k, bands * lev_count - 1)
            slots_out[d, k] = rows_in[rank % lev_count, rank // lev_count]
        start = start + held_here
    for offset in range(1, lat_count):
        target = lat_peer(offset)
        pltpu.make_async_remote_copy(
            src_ref=slots_out.at[target],
            dst_ref=slots_in.at[me],
            send_sem=d_send,
            recv_sem=d_recv,
            device_id={"lat": target},
            device_id_type=pl.DeviceIdType.MESH,
        ).start()
    slots_in[me] = slots_out[me]
    settle(slots_in.at[pl.ds(0, lat_count - 1)], d_recv)

    def finish(k, carry):
        for o in range(lat_count):
            offset = k * lat_count + o
            wavenumber = mine + offset
            divisor = ((members - 1) * (2 * wavenumber + 2)).astype(jnp.float32)
            chosen = slots_in[wavenumber % lat_count, k].astype(jnp.float32) / divisor
            out_ref[offset] = jnp.where(offset < count, chosen, jnp.zeros_like(chosen))
        return carry

    lax.fori_loop(0, share, finish, 0)
    settle(part_out.at[:, pl.ds(0, lat_count - 1)], p_send)
    settle(rows_out.at[pl.ds(0, lev_count - 1)], l_send)
    settle(slots_out.at[pl.ds(0, lat_count - 1)], d_send)
    settle(sent.at[pl.ds(0, lat_count - 1)], s_send)
    for i in range(blocks):
        for part in columns[i]:
            settle(table_remote(i, part), t_send.at[part[2]])
            if part[2] in shared:
                settle(table_passed(i, part), w_send.at[part[2]])

        def drain(t, carry):
            for_waves(i, t, lambda copy: copy.wait_send())
            return carry

        lax.fori_loop(block_of(i, me, lat_count) // lev_count, bands, drain, 0)


def on_device(lat_count, lev_count, fields, legendre, owner_counts):
    members, lev_rows, lat_rows, points = fields.shape
    modes, totals = legendre.shape[1:]
    rows = members * lev_rows
    groups = rows // LANES
    blocks = modes // (SUB * lat_count)
    bands = totals // (SUB * lev_count)
    levels = lev_count * lev_rows
    span = 2 * SUB
    steps = lat_rows // span * groups
    starts = [block_of(i, j, lat_count) * SUB for j in range(lat_count) for i in range(blocks)]
    orders = np.concatenate([np.array(starts) + r for r in range(SUB)])
    tables = [jnp.asarray(t) for t in folded_tables(points, orders)]
    places = sum(bands - i * lat_count // lev_count for i in range(blocks))
    widths = [totals - i * lat_count * SUB // LANES * LANES for i in range(blocks)]
    wide = max(2 * points, 2 * groups * totals + totals // LANES * lat_count * lat_rows)
    size = (lat_count, lev_count, members, lev_rows, totals, blocks)
    vmem = pl.BlockSpec(memory_space=pltpu.VMEM)
    hbm = pl.BlockSpec(memory_space=pl.ANY)
    smem = pl.BlockSpec(memory_space=pltpu.SMEM)
    capacity = 2 * modes // owner_counts.shape[0]
    share = capacity // lat_count
    return pl.pallas_call(
        functools.partial(main_kernel, size),
        out_shape=jax.ShapeDtypeStruct((capacity, lev_rows, levels), jnp.float32),
        in_specs=[smem, hbm, hbm, vmem, vmem, vmem],
        out_specs=vmem,
        scratch_shapes=[pltpu.VMEM((lat_count, lat_rows, SUB, w), jnp.bfloat16) for w in widths]
        + [
            pltpu.VMEM((wide, SUB, LANES), jnp.float32),
            pltpu.VMEM((2, modes * span, LANES), jnp.float32),
            pltpu.VMEM((lat_count, blocks, steps, SUB, span, 2 * LANES), jnp.bfloat16),
            pltpu.VMEM((blocks, lat_count, steps, SUB, span, 2 * LANES), jnp.bfloat16),
            pltpu.VMEM((places, lev_count, SUB * SUB, 2 * rows), jnp.bfloat16),
            pltpu.VMEM((places, lev_count, SUB * SUB, 2 * rows), jnp.bfloat16),
            pltpu.VMEM((SUB, 2 * groups * (LANES // lev_rows), SUB, LANES), jnp.float32),
            pltpu.VMEM((bands, lat_count, levels, levels), jnp.bfloat16),
            pltpu.VMEM((bands, lat_count, levels, levels), jnp.bfloat16),
            pltpu.VMEM((lev_count, bands, lev_rows, levels), jnp.bfloat16),
            pltpu.VMEM((lev_count, bands, lev_rows, levels), jnp.bfloat16),
            pltpu.VMEM((lat_count, share, lev_rows, levels), jnp.bfloat16),
            pltpu.VMEM((lat_count, share, lev_rows, levels), jnp.bfloat16),
            pltpu.SemaphoreType.DMA((2,)),
            pltpu.SemaphoreType.DMA((2 * blocks + 1,)),
            pltpu.SemaphoreType.DMA((blocks + 1,)),
            pltpu.SemaphoreType.DMA((blocks + 1,)),
            pltpu.SemaphoreType.DMA,
            pltpu.SemaphoreType.DMA((blocks,)),
            pltpu.SemaphoreType.DMA((places, lev_count - 1)),
            pltpu.SemaphoreType.DMA((places,)),
            pltpu.SemaphoreType.DMA,
            pltpu.SemaphoreType.DMA((bands,)),
            pltpu.SemaphoreType.DMA,
            pltpu.SemaphoreType.DMA,
            pltpu.SemaphoreType.DMA,
            pltpu.SemaphoreType.DMA,
            pltpu.SemaphoreType.DMA((blocks + 1,)),
            pltpu.SemaphoreType.DMA((blocks + 1,)),
        ],
        compiler_params=pltpu.CompilerParams(
            vmem_limit_bytes=VMEM_LIMIT, collective_id=0, has_side_effects=True
        ),
        cost_estimate=pl.CostEstimate(flops=40_000_000_000, bytes_accessed=80_000_000, transcendentals=0),
    )(owner_counts, fields.reshape(rows, lat_rows // SUB, SUB, points), legendre, *tables)


def pick(lat_count, lev_count, fields, legendre, owner_counts):
    members, lev_rows, lat_rows, points = fields.shape
    modes = legendre.shape[1]
    fits = (
        lat_rows % 16 == 0
        and lat_rows % lev_count == 0
        and members * lev_rows % LANES == 0
        and lev_rows * lev_count == LANES
        and lat_count == SUB
        and modes % (2 * SUB * lat_count) == 0
        and owner_counts.shape[0] == lat_count
        and 2 * modes // lat_count % lat_count == 0
        and legendre.shape[2] <= 2 * modes
        and modes % (lat_count * lev_count) == 0
    )
    if fits:
        return on_device(lat_count, lev_count, fields, legendre, owner_counts)
    return plain_on_device(fields, legendre, owner_counts)


def solution(mesh):
    return jax.shard_map(
        functools.partial(pick, mesh.shape["lat"], mesh.shape["lev"]),
        mesh=mesh,
        in_specs=(P(None, "lev", "lat", None), P("lat", None, None), P()),
        out_specs=P("lat", "lev", None),
        check_vma=False,
    )
```
